128 devices in a mesh: row: 16 (over z_lo, x, core), col: 8 (over z_hi, y).
Axes of the slice: x: 4, y: 4, z: 4 (z_hi: 2, z_lo: 2; z = z_hi * 2 + z_lo), core: 2. Of those that a mesh axis runs over, the one named last changes fastest.
Arguments:
- density: bfloat16 [64, 5, 256, 256], P('row', None, 'col'), may hold values from -1 to 2, as said below
- pattern: int32 [64, 5], P('row'), may hold values from 0 to 1, as said below
- windows: int32 [256], P(('row', 'col')), may hold values from 0 to 125, as said below
- basis_values: bfloat16 [256, 4096, 384], P(('row', 'col')), may hold values from -6 to 6
- basis_grads: bfloat16 [3, 256, 4096, 384], P(None, ('row', 'col')), may hold values from -48 to 48
- weights: float32 [256, 4096], P(('row', 'col')), may hold values from 0.25 to 4
Outputs:
- purified: bfloat16 [64, 5, 256, 256], P('row', None, 'col')
- xc_matrix: float32 [64, 5, 256, 256], P('row', None, 'col')
- grid_density: float32 [256, 4096], P(('row', 'col'))
The draws below stay inside these ranges and needn't reach their ends.
Inputs may be any that keep to these rules, and one draw needn't show every extreme that they name: density[i, d] is block (i, i + d - 2) of a symmetric matrix: density[i, d] equals density[i + d - 2, 4 - d] transposed; blocks whose column block lies outside the matrix are 0. pattern[i, d] = pattern[i + d - 2, 4 - d]; it is 1 for d = 1, 2, 3 where block i + d - 2 exists and 0 where it does not. Tile t lies on device t // 2 of the joined axes row+col; if that device has row index q, windows[t] lies between 2 * 4 q - 2 and 2 * 4 q + 2 * 4 - 1.
All inputs are finite; a program needn't handle non-finite values.
Results may differ from the reference program's by a relative error of at most 0.011.
Values may be sent and summed in bfloat16 or wider, within the bound.
A program may use at most 128 MiB of HBM per device.

```python
import math
import jax
import jax.numpy as jnp
from jax import lax

BS = 256
HB = 128
FN = 384
BD = 4
BLOCKS = 64
TILES_DEV = 2
POINTS = 4096
NTILES = 256
ITERS = 2
N_COL = 8


def draw_density(key, part):
    noise_key = jax.random.fold_in(key, 11)
    diag_key = jax.random.fold_in(key, 12)
    noise = jnp.clip(jax.random.normal(noise_key, (BLOCKS, 5, BS, BS), jnp.float32), -4.0, 4.0)
    level = 0.6
    diagonal = jax.random.uniform(diag_key, (BLOCKS, BS), jnp.float32, 0.2, 0.8)
    padded = jnp.pad(noise, ((2, 2), (0, 0), (0, 0), (0, 0)))
    partners = jnp.stack([jnp.swapaxes(padded[band:band + BLOCKS, 4 - band], 1, 2) for band in range(5)], axis=1)
    symmetric = (noise + partners) * (0.5 * level / jnp.sqrt(jnp.float32(5 * BS)))
    block_ids = jnp.arange(BLOCKS, dtype=jnp.int32)[:, None]
    band_ids = jnp.arange(5, dtype=jnp.int32)[None, :]
    partner_ids = block_ids + band_ids - 2
    valid = ((partner_ids >= 0) & (partner_ids < BLOCKS))[:, :, None, None]
    identity = jnp.eye(BS, dtype=jnp.float32)[None, None]
    centre = (band_ids == 2)[:, :, None, None]
    filled = jnp.where(centre, symmetric * (1.0 - identity) + identity * diagonal[:, None, None, :], symmetric)
    return jnp.where(valid, filled, 0.0).astype(jnp.bfloat16)


def draw_pattern(key, part):
    picks = jax.random.randint(jax.random.fold_in(key, 21), (BLOCKS,), 0, 2)
    block_ids = jnp.arange(BLOCKS, dtype=jnp.int32)[:, None]
    band_ids = jnp.arange(5, dtype=jnp.int32)[None, :]
    partner_ids = block_ids + band_ids - 2
    valid = (partner_ids >= 0) & (partner_ids < BLOCKS)
    earlier = jnp.roll(picks, 2)[:, None]
    far = jnp.where(band_ids == 4, picks[:, None], jnp.where(band_ids == 0, earlier, 0))
    near = jnp.abs(band_ids - 2) <= 1
    return jnp.where(valid, jnp.where(near, 1, far), 0).astype(jnp.int32)


def draw_windows(key, part):
    tiles_idx = jnp.arange(NTILES, dtype=jnp.int32)
    row_of = tiles_idx // TILES_DEV // N_COL
    lowest = jnp.maximum(0, 2 * BD * row_of - 2)
    highest = jnp.minimum(2 * BLOCKS - 3, 2 * BD * row_of + 2 * BD - 1)
    picks = jax.random.randint(jax.random.fold_in(key, 31), (NTILES,), 0, 1 << 20)
    return (lowest + picks % (highest - lowest + 1)).astype(jnp.int32)


def steps_of(key, shape, cuts, least, high):
    level = 1.0
    for dim, blocks in cuts:
        heights = jax.random.uniform(jax.random.fold_in(jax.random.fold_in(key, 6), dim), (blocks,), jnp.float32, least / len(cuts), high / len(cuts))
        level = level * jnp.repeat(jnp.exp(heights), shape[dim] // blocks).reshape((-1,) + (1,) * (len(shape) - 1 - dim))
    return level


def gaussian(key, dims, scale, most, shards=(), held_as=jnp.bfloat16):
    values = scale * jax.random.normal(key, dims, jnp.float32)
    if shards:
        values = values * steps_of(key, dims, shards, -0.22, 0.18)
    return jnp.clip(values, -most, most).astype(held_as)


def setup_inputs(seed: int = 0) -> dict:
    key_list = jax.random.split(jax.random.key(seed), 7)
    density = draw_density(jax.random.fold_in(key_list[6], 71), 0)
    pattern = draw_pattern(jax.random.fold_in(key_list[6], 71), 0)
    windows = draw_windows(jax.random.fold_in(key_list[6], 71), 0)
    basis_values = gaussian(key_list[3], (NTILES, POINTS, FN), 1.0, 6.0, ((0, 128),))
    basis_grads = gaussian(key_list[4], (3, NTILES, POINTS, FN), 8.0, 48.0, ((1, 128),))
    weights = jnp.clip(jnp.exp(math.log(4.0) - 2.7725887 * jax.random.uniform(key_list[5], (NTILES, POINTS), jnp.float32) ** steps_of(key_list[5], (NTILES, POINTS), ((0, 128),), -0.2, 0.2)), 0.25, 4.0)
    return dict(density=density, pattern=pattern, windows=windows, basis_values=basis_values, basis_grads=basis_grads, weights=weights)


slater_cx = 0.7386
kappa_pbe = 0.804
mu_pbe = 0.2195

def energy_sum(point_density, grad_square):
    spread = jnp.sqrt(point_density * point_density + 1.0)
    reduced = grad_square / spread ** (8.0 / 3.0)
    enhance = 1.0 + kappa_pbe - kappa_pbe / (1.0 + mu_pbe * reduced / kappa_pbe)
    return jnp.sum(-slater_cx * spread ** (4.0 / 3.0) * enhance)

def tile_terms(values, grads, quadrature, window_block):
    functions = values.shape[1]
    points = values.shape[0]
    projected = jnp.dot(values, window_block, preferred_element_type=jnp.float32)
    point_density = lax.optimization_barrier(jnp.sum(projected * values.astype(jnp.float32), axis=1)) / functions
    slopes = 2.0 * lax.optimization_barrier(jnp.sum(projected[None] * grads.astype(jnp.float32), axis=2)) / functions
    grad_square = lax.optimization_barrier(jnp.sum(slopes * slopes, axis=0))
    by_density, by_gradient = jax.grad(energy_sum, argnums=(0, 1))(point_density, grad_square)
    scaled = quadrature / points
    weighted = (0.5 * by_density * scaled)[:, None] * values.astype(jnp.float32)
    weighted = weighted + lax.optimization_barrier(jnp.sum(((2.0 * by_gradient * scaled)[None] * slopes)[:, :, None] * grads.astype(jnp.float32), axis=0))
    weighted = weighted.astype(jnp.bfloat16)
    one_side = lax.dot_general(values, weighted, (((0,), (0,)), ((), ())), preferred_element_type=jnp.float32)
    return (point_density, one_side + one_side.T)

def band_product(left, right_padded):
    blocks = left.shape[0]
    total = None
    for offset_step in range(5):
        shifted = right_padded[offset_step:offset_step + blocks]
        widened = jnp.pad(shifted, ((0, 0), (2, 2), (0, 0), (0, 0)))
        picked = widened[:, 4 - offset_step:9 - offset_step]
        term = jnp.einsum('brk,bdkc->bdrc', left[:, offset_step].astype(jnp.float32), picked.astype(jnp.float32))
        total = term if total is None else total + term
    return total

def window_of(band_three, lead, offset, functions):
    paired = lax.dynamic_slice_in_dim(band_three, lead, 2, 0)
    upper = jnp.concatenate([paired[0, 1], paired[0, 2]], axis=1)
    lower = jnp.concatenate([paired[1, 0], paired[1, 1]], axis=1)
    dense = jnp.concatenate([upper, lower], axis=0)
    return lax.dynamic_slice(dense, (offset, offset), (functions, functions))

def spread_term(summed, term, lead, offset):
    width = summed.shape[2]
    dense = lax.dynamic_update_slice(jnp.zeros((2 * width, 2 * width), summed.dtype), term.astype(summed.dtype), (offset, offset))
    nothing = jnp.zeros((width, width), summed.dtype)
    upper = jnp.stack([nothing, dense[:width, :width], dense[:width, width:]])
    lower = jnp.stack([dense[width:, :width], dense[width:, width:], nothing])
    increment = jnp.stack([upper, lower])
    paired = lax.dynamic_slice_in_dim(summed, lead, 2, 0)
    return lax.dynamic_update_slice_in_dim(summed, paired + increment, lead, 0)

def reference(density, pattern, windows, basis_values, basis_grads, weights):
    kept = (pattern > 0)[:, :, None, None]
    current = jnp.where(kept, density, jnp.zeros_like(density))
    for iteration in range(ITERS):
        padded = jnp.pad(current, ((2, 2), (0, 0), (0, 0), (0, 0)))
        square = jnp.where(kept, band_product(current, padded), 0.0).astype(jnp.bfloat16)
        cubic = band_product(square, padded)
        current = jnp.where(kept, 3.0 * square.astype(jnp.float32) - 2.0 * cubic, 0.0).astype(jnp.bfloat16)
    near = current[:, 1:4]

    def one_tile(tile_index, carry):
        summed, densities = carry
        position = tile_index.astype(jnp.int32)
        start_step = windows[position]
        lead = (start_step // 2).astype(jnp.int32)
        offset = (start_step % 2 * HB).astype(jnp.int32)
        window_block = window_of(near, lead, offset, FN)
        values = lax.dynamic_index_in_dim(basis_values, position, 0, keepdims=False)
        grads = lax.dynamic_index_in_dim(basis_grads, position, 1, keepdims=False)
        quadrature = lax.dynamic_index_in_dim(weights, position, 0, keepdims=False)
        point_density, contribution = tile_terms(values, grads, quadrature, window_block)
        summed = spread_term(summed, contribution, lead, offset)
        densities = lax.dynamic_update_index_in_dim(densities, point_density, position, 0)
        return (summed, densities)
    start_carry = (jnp.zeros((BLOCKS, 3, BS, BS), jnp.float32), jnp.zeros((NTILES, POINTS), jnp.float32))
    summed, densities = lax.fori_loop(0, NTILES, one_tile, start_carry)
    xc_matrix = jnp.where(kept, jnp.pad(summed, ((0, 0), (1, 1), (0, 0), (0, 0))), 0.0)
    return (current, xc_matrix, densities)
```

```python
import jax
import jax.numpy as jnp
from jax import lax
from jax.experimental import pallas as pl
from jax.experimental.pallas import tpu as pltpu
from jax.sharding import Mesh
from jax.sharding import PartitionSpec as P

ITERS = 2
COL = ("col_0", "col_1")
ROW_COL = ("row", "col_0", "col_1")


slater_cx = 0.7386
kappa_pbe = 0.804
mu_pbe = 0.2195


def shifted_2(value, axis, by):
    length = lax.axis_size(axis)
    pairs = [(i, i + by) for i in range(length) if 0 <= i + by < length]
    return lax.ppermute(value, axis, pairs)


def padded(cells, sides, width):
    for axis, dim in sides:
        count = lax.axis_size(axis)
        ends = count - 1
        head = lax.slice_in_dim(cells, 0, width, axis=dim)
        tail = lax.slice_in_dim(cells, cells.shape[dim] - width, cells.shape[dim], axis=dim)
        cells = jnp.concatenate(
            [
                lax.ppermute(tail, axis, [(i, (i + 1) % count) for i in range(ends)]),
                cells,
                lax.ppermute(head, axis, [((i + 1) % count, i) for i in range(ends)]),
            ],
            axis=dim,
        )
    return cells


def in_order(pieces, dim):
    pieces = jnp.moveaxis(pieces, 0, dim)
    lengths = pieces.shape
    return pieces.reshape(*lengths[:dim], lengths[dim] * lengths[dim + 1], *lengths[dim + 2 :])


def sent_to_all(value, axis):
    length = lax.axis_size(axis)
    return lax.all_to_all(
        jnp.broadcast_to(value[None], (length, *value.shape)), axis, 0, 0, tiled=True
    )


def gather_directly(value, axis, dim):
    return in_order(sent_to_all(value, axis), dim)


def sum_in_order(pieces, axes, sequence):
    inside = pieces.shape[1:]
    pieces = pieces.reshape(*(lax.axis_size(a) for a in axes), *inside)
    pieces = jnp.moveaxis(pieces, sequence, range(len(axes))).reshape(-1, *inside)
    for k in sequence:
        pieces = lax.psum_scatter(pieces, axes[k], scatter_dimension=0, tiled=True)
    return pieces[0]


def cut_along(value, dim, length):
    before, after = (value.shape[:dim], value.shape[dim + 1 :])
    return jnp.moveaxis(value.reshape(*before, length, -1, *after), dim, 0)


def scatter_axes(value, axes, sequence, dim):
    length = lax.axis_size(axes)
    return sum_in_order(cut_along(value, dim, length), axes, sequence)


POINT_BLOCK = 1024
CHUNK = 128


def potentials(density, grad_square):
    inverse_root = jnp.exp(jnp.log(density * density + 1.0) * (-1.0 / 3.0))
    inverse_two = inverse_root * inverse_root
    reduced = grad_square * (inverse_two * inverse_two)
    share = 1.0 / (1.0 + (mu_pbe / kappa_pbe) * reduced)
    enhance = 1.0 + kappa_pbe - kappa_pbe * share
    slope = mu_pbe * share * share
    by_density = (-slater_cx * 4.0 / 3.0) * inverse_root * density * (enhance - 2.0 * reduced * slope)
    by_gradient = -slater_cx * slope * inverse_two
    return by_density, by_gradient


def tile_kernel(window_ref, values_ref, grads_ref, weights_ref, density_ref, term_ref, projected, weighted, total):
    step = pl.program_id(1)
    functions = values_ref.shape[2]
    projected[...] = jnp.dot(values_ref[0], window_ref[0], preferred_element_type=jnp.float32)
    lane = lax.broadcasted_iota(jnp.int32, (8, 128), 1)
    packed = [jnp.zeros((8, 128), jnp.float32) for _ in range(4)]
    for chunk in range(POINT_BLOCK // CHUNK):
        rows = slice(chunk * CHUNK, (chunk + 1) * CHUNK)
        x = projected[rows, :]
        for k in range(4):
            basis = values_ref[0, rows, :] if k == 0 else grads_ref[k - 1, 0, rows, :]
            sums = jnp.sum(x * basis.astype(jnp.float32), axis=1, keepdims=True)
            for group in range(CHUNK // 8):
                here = chunk * (CHUNK // 8) + group
                packed[k] = jnp.where(lane == here, sums[8 * group : 8 * group + 8], packed[k])
    density = packed[0] / functions
    slopes = [2.0 * packed[k] / functions for k in (1, 2, 3)]
    grad_square = slopes[0] * slopes[0] + slopes[1] * slopes[1] + slopes[2] * slopes[2]
    by_density, by_gradient = potentials(density, grad_square)
    density_ref[0, 0] = density
    scaled = weights_ref[0, 0] * (1.0 / 4096.0)
    factors = [0.5 * by_density * scaled] + [2.0 * by_gradient * scaled * s for s in slopes]
    for pair in range(POINT_BLOCK // 16):
        rows = slice(pair * 16, pair * 16 + 16)
        z = None
        for k in range(4):
            basis = values_ref[0, rows, :] if k == 0 else grads_ref[k - 1, 0, rows, :]
            column = jnp.concatenate(
                [factors[k][:, 2 * pair : 2 * pair + 1], factors[k][:, 2 * pair + 1 : 2 * pair + 2]], axis=0
            )
            part = column * basis.astype(jnp.float32)
            z = part if z is None else z + part
        weighted[rows, :] = z.astype(jnp.bfloat16)
    one_side = lax.dot_general(
        values_ref[0], weighted[...], (((0,), (0,)), ((), ())), preferred_element_type=jnp.float32
    )

    @pl.when(step == 0)
    def _():
        total[...] = one_side

    @pl.when(step > 0)
    def _():
        total[...] += one_side

    @pl.when(step == pl.num_programs(1) - 1)
    def _():
        term_ref[0] = total[...] + total[...].T


def tile_terms(values, grads, quadrature, window_blocks):
    tiles, points, functions = values.shape
    steps = points // POINT_BLOCK
    packed_weights = jnp.swapaxes(quadrature.reshape(tiles, steps, 128, 8), 2, 3)
    density, terms = pl.pallas_call(
        tile_kernel,
        name="tile_terms",
        grid=(tiles, steps),
        in_specs=[
            pl.BlockSpec((1, functions, functions), lambda t, s: (t, 0, 0)),
            pl.BlockSpec((1, POINT_BLOCK, functions), lambda t, s: (t, s, 0)),
            pl.BlockSpec((3, 1, POINT_BLOCK, functions), lambda t, s: (0, t, s, 0)),
            pl.BlockSpec((1, 1, 8, 128), lambda t, s: (t, s, 0, 0)),
        ],
        out_specs=[
            pl.BlockSpec((1, 1, 8, 128), lambda t, s: (t, s, 0, 0)),
            pl.BlockSpec((1, functions, functions), lambda t, s: (t, 0, 0)),
        ],
        out_shape=[
            jax.ShapeDtypeStruct((tiles, steps, 8, 128), jnp.float32),
            jax.ShapeDtypeStruct((tiles, functions, functions), jnp.float32),
        ],
        scratch_shapes=[
            pltpu.VMEM((POINT_BLOCK, functions), jnp.float32),
            pltpu.VMEM((POINT_BLOCK, functions), jnp.bfloat16),
            pltpu.VMEM((functions, functions), jnp.float32),
        ],
        compiler_params=pltpu.CompilerParams(
            dimension_semantics=("arbitrary", "arbitrary"), vmem_limit_bytes=40 * 1024 * 1024
        ),
        cost_estimate=pl.CostEstimate(
            flops=4 * tiles * points * functions * functions,
            bytes_accessed=8 * tiles * points * functions,
            transcendentals=0,
        ),
    )(window_blocks, values, grads, packed_weights)
    return jnp.swapaxes(density, 2, 3).reshape(tiles, points), terms


def band_product(left, right_padded):
    blocks = left.shape[0]
    total = None
    for offset_step in range(5):
        shifted = right_padded[offset_step : offset_step + blocks]
        widened = jnp.pad(shifted, ((0, 0), (2, 2), (0, 0), (0, 0)))
        picked = widened[:, 4 - offset_step : 9 - offset_step]
        term = jnp.einsum(
            "brk,bdkc->bdrc", left[:, offset_step], picked, preferred_element_type=jnp.float32
        )
        total = term if total is None else total + term
    return total


def window_of(band_three, lead, offset, functions):
    paired = lax.dynamic_slice_in_dim(band_three, lead, 2, 0)
    upper = jnp.concatenate([paired[0, 1], paired[0, 2]], axis=1)
    lower = jnp.concatenate([paired[1, 0], paired[1, 1]], axis=1)
    dense = jnp.concatenate([upper, lower], axis=0)
    return lax.dynamic_slice(dense, (offset, offset), (functions, functions))


def spread_term(summed, term, lead, offset):
    width = summed.shape[2]
    dense = lax.dynamic_update_slice(
        jnp.zeros((2 * width, 2 * width), summed.dtype), term, (offset, offset)
    )
    nothing = jnp.zeros((width, width), summed.dtype)
    upper = jnp.stack([nothing, dense[:width, :width], dense[:width, width:]])
    lower = jnp.stack([dense[width:, :width], dense[width:, width:], nothing])
    increment = jnp.stack([upper, lower])
    paired = lax.dynamic_slice_in_dim(summed, lead, 2, 0)
    return lax.dynamic_update_slice_in_dim(summed, paired + increment, lead, 0)


def edge_rows(summed):
    blocks = summed.shape[0] - 2
    from_above = shifted_2(summed[0].astype(jnp.bfloat16), "row", -1).astype(jnp.float32)
    from_below = shifted_2(summed[blocks + 1].astype(jnp.bfloat16), "row", 1).astype(jnp.float32)
    own_rows = summed[1 : blocks + 1]
    return jnp.concatenate(
        [
            own_rows[:1] + from_below[None],
            own_rows[1 : blocks - 1],
            own_rows[blocks - 1 :] + from_above[None],
        ],
        axis=0,
    )


def on_device(density, pattern, windows, basis_values, basis_grads, weights):
    row_index = lax.axis_index("row")
    band_rows = density.shape[0]
    functions = basis_values.shape[2]
    step_size = functions // 3
    kept = (pattern > 0)[:, :, None, None]
    current = jnp.where(kept, density, jnp.zeros_like(density))
    for iteration in range(ITERS):
        near_right = padded(current, (("row", 0),), 2)
        right_full = lax.all_gather(near_right, COL, axis=2, tiled=True)
        square = jnp.where(kept, band_product(current, right_full), 0.0).astype(jnp.bfloat16)
        cubic = band_product(square, right_full)
        current = jnp.where(kept, 3.0 * square.astype(jnp.float32) - 2.0 * cubic, 0.0).astype(
            jnp.bfloat16
        )
    rows_band = gather_directly(current[:, 1:4], COL, 2)
    near = padded(rows_band, (("row", 0),), 1)
    tiles_here = windows.shape[0]
    block_size = near.shape[2]
    leads = [windows[t] // 2 - (band_rows * row_index - 1) for t in range(tiles_here)]
    offsets = [windows[t] % 2 * step_size for t in range(tiles_here)]
    window_blocks = jnp.stack(
        [window_of(near, leads[t], offsets[t], functions) for t in range(tiles_here)]
    )
    densities, contributions = tile_terms(basis_values, basis_grads, weights, window_blocks)
    local_terms = jnp.zeros((band_rows + 2, 3, block_size, block_size), jnp.float32)
    for t in range(tiles_here):
        local_terms = spread_term(local_terms, contributions[t], leads[t], offsets[t])
    owner_part = scatter_axes(local_terms.astype(jnp.bfloat16), COL, (1, 0), 2).astype(jnp.float32)
    mine = edge_rows(owner_part)
    xc_matrix = jnp.where(kept, jnp.pad(mine, ((0, 0), (1, 1), (0, 0), (0, 0))), 0.0)
    return (current, xc_matrix, densities)


def solution(mesh):
    torus = Mesh(mesh.devices.reshape(mesh.shape["row"], 2, 4), ("row", "col_0", "col_1"))
    placed = (
        P("row", None, COL, None),
        P("row", None),
        P(ROW_COL),
        P(ROW_COL, None, None),
        P(None, ROW_COL, None, None),
        P(ROW_COL, None),
    )
    return jax.shard_map(
        on_device,
        mesh=torus,
        in_specs=placed,
        out_specs=(P("row", None, COL, None), P("row", None, COL, None), P(ROW_COL, None)),
        check_vma=False,
    )
```

```python
import jax
import jax.numpy as jnp
from jax import lax
from jax.experimental import pallas as pl
from jax.experimental.pallas import tpu as pltpu
from jax.sharding import PartitionSpec as P

ITERS = 2
COL = "col"
ROW_COL = ("row", "col")


slater_cx = 0.7386
kappa_pbe = 0.804
mu_pbe = 0.2195


def shifted_2(value, axis, by):
    length = lax.axis_size(axis)
    pairs = [(i, i + by) for i in range(length) if 0 <= i + by < length]
    return lax.ppermute(value, axis, pairs)


def padded(cells, sides, width):
    for axis, dim in sides:
        count = lax.axis_size(axis)
        ends = count - 1
        head = lax.slice_in_dim(cells, 0, width, axis=dim)
        tail = lax.slice_in_dim(cells, cells.shape[dim] - width, cells.shape[dim], axis=dim)
        cells = jnp.concatenate(
            [
                lax.ppermute(tail, axis, [(i, (i + 1) % count) for i in range(ends)]),
                cells,
                lax.ppermute(head, axis, [((i + 1) % count, i) for i in range(ends)]),
            ],
            axis=dim,
        )
    return cells


def in_order(pieces, dim):
    pieces = jnp.moveaxis(pieces, 0, dim)
    lengths = pieces.shape
    return pieces.reshape(*lengths[:dim], lengths[dim] * lengths[dim + 1], *lengths[dim + 2 :])


def sent_to_all(value, axis):
    length = lax.axis_size(axis)
    return lax.all_to_all(
        jnp.broadcast_to(value[None], (length, *value.shape)), axis, 0, 0, tiled=True
    )


def gather_directly(value, axis, dim):
    return in_order(sent_to_all(value, axis), dim)


def sum_in_order(pieces, axes, sequence):
    inside = pieces.shape[1:]
    pieces = pieces.reshape(*(lax.axis_size(a) for a in axes), *inside)
    pieces = jnp.moveaxis(pieces, sequence, range(len(axes))).reshape(-1, *inside)
    for k in sequence:
        pieces = lax.psum_scatter(pieces, axes[k], scatter_dimension=0, tiled=True)
    return pieces[0]


def cut_along(value, dim, length):
    before, after = (value.shape[:dim], value.shape[dim + 1 :])
    return jnp.moveaxis(value.reshape(*before, length, -1, *after), dim, 0)


def scatter_axes(value, axes, sequence, dim):
    length = lax.axis_size(axes)
    return sum_in_order(cut_along(value, dim, length), axes, sequence)


POINT_BLOCK = 1024
CHUNK = 128


def potentials(density, grad_square):
    inverse_root = jnp.exp(jnp.log(density * density + 1.0) * (-1.0 / 3.0))
    inverse_two = inverse_root * inverse_root
    reduced = grad_square * (inverse_two * inverse_two)
    share = 1.0 / (1.0 + (mu_pbe / kappa_pbe) * reduced)
    enhance = 1.0 + kappa_pbe - kappa_pbe * share
    slope = mu_pbe * share * share
    by_density = (-slater_cx * 4.0 / 3.0) * inverse_root * density * (enhance - 2.0 * reduced * slope)
    by_gradient = -slater_cx * slope * inverse_two
    return by_density, by_gradient


def tile_kernel(window_ref, values_ref, grads_ref, weights_ref, density_ref, term_ref, projected, weighted, total):
    step = pl.program_id(1)
    functions = values_ref.shape[2]
    projected[...] = jnp.dot(values_ref[0], window_ref[0], preferred_element_type=jnp.float32)
    lane = lax.broadcasted_iota(jnp.int32, (8, 128), 1)
    packed = [jnp.zeros((8, 128), jnp.float32) for _ in range(4)]
    for chunk in range(POINT_BLOCK // CHUNK):
        rows = slice(chunk * CHUNK, (chunk + 1) * CHUNK)
        x = projected[rows, :]
        for k in range(4):
            basis = values_ref[0, rows, :] if k == 0 else grads_ref[k - 1, 0, rows, :]
            sums = jnp.sum(x * basis.astype(jnp.float32), axis=1, keepdims=True)
            for group in range(CHUNK // 8):
                here = chunk * (CHUNK // 8) + group
                packed[k] = jnp.where(lane == here, sums[8 * group : 8 * group + 8], packed[k])
    density = packed[0] / functions
    slopes = [2.0 * packed[k] / functions for k in (1, 2, 3)]
    grad_square = slopes[0] * slopes[0] + slopes[1] * slopes[1] + slopes[2] * slopes[2]
    by_density, by_gradient = potentials(density, grad_square)
    density_ref[0, 0] = density
    scaled = weights_ref[0, 0] * (1.0 / 4096.0)
    factors = [0.5 * by_density * scaled] + [2.0 * by_gradient * scaled * s for s in slopes]
    for pair in range(POINT_BLOCK // 16):
        rows = slice(pair * 16, pair * 16 + 16)
        z = None
        for k in range(4):
            basis = values_ref[0, rows, :] if k == 0 else grads_ref[k - 1, 0, rows, :]
            column = jnp.concatenate(
                [factors[k][:, 2 * pair : 2 * pair + 1], factors[k][:, 2 * pair + 1 : 2 * pair + 2]], axis=0
            )
            part = column * basis.astype(jnp.float32)
            z = part if z is None else z + part
        weighted[rows, :] = z.astype(jnp.bfloat16)
    one_side = lax.dot_general(
        values_ref[0], weighted[...], (((0,), (0,)), ((), ())), preferred_element_type=jnp.float32
    )

    @pl.when(step == 0)
    def _():
        total[...] = one_side

    @pl.when(step > 0)
    def _():
        total[...] += one_side

    @pl.when(step == pl.num_programs(1) - 1)
    def _():
        term_ref[0] = total[...] + total[...].T


def tile_terms(values, grads, quadrature, window_blocks):
    tiles, points, functions = values.shape
    steps = points // POINT_BLOCK
    packed_weights = jnp.swapaxes(quadrature.reshape(tiles, steps, 128, 8), 2, 3)
    density, terms = pl.pallas_call(
        tile_kernel,
        name="tile_terms",
        grid=(tiles, steps),
        in_specs=[
            pl.BlockSpec((1, functions, functions), lambda t, s: (t, 0, 0)),
            pl.BlockSpec((1, POINT_BLOCK, functions), lambda t, s: (t, s, 0)),
            pl.BlockSpec((3, 1, POINT_BLOCK, functions), lambda t, s: (0, t, s, 0)),
            pl.BlockSpec((1, 1, 8, 128), lambda t, s: (t, s, 0, 0)),
        ],
        out_specs=[
            pl.BlockSpec((1, 1, 8, 128), lambda t, s: (t, s, 0, 0)),
            pl.BlockSpec((1, functions, functions), lambda t, s: (t, 0, 0)),
        ],
        out_shape=[
            jax.ShapeDtypeStruct((tiles, steps, 8, 128), jnp.float32),
            jax.ShapeDtypeStruct((tiles, functions, functions), jnp.float32),
        ],
        scratch_shapes=[
            pltpu.VMEM((POINT_BLOCK, functions), jnp.float32),
            pltpu.VMEM((POINT_BLOCK, functions), jnp.bfloat16),
            pltpu.VMEM((functions, functions), jnp.float32),
        ],
        compiler_params=pltpu.CompilerParams(
            dimension_semantics=("arbitrary", "arbitrary"), vmem_limit_bytes=40 * 1024 * 1024
        ),
        cost_estimate=pl.CostEstimate(
            flops=4 * tiles * points * functions * functions,
            bytes_accessed=8 * tiles * points * functions,
            transcendentals=0,
        ),
    )(window_blocks, values, grads, packed_weights)
    return jnp.swapaxes(density, 2, 3).reshape(tiles, points), terms


BLOCKS = 64
BAND = 5
HALF = 128
WIDTH = 256
SLICE = 32
COLS = 8
FIRST_PIECES = {
    -2: ((2, 2, 0),),
    -1: ((2, 1, 2), (4, 1, 3)),
    0: ((0, 5, 4),),
    1: ((2, 2, 9),),
    2: ((2, 1, 11),),
}
FIRST_ROLE = {-2: (0, 2), -1: (2, 2), 0: (4, 5), 1: (9, 2), 2: (11, 1)}
FIRST_SLOT = {(-2, -2): 0, (-2, -1): 1, (-1, -1): 2, (-1, 1): 3, (1, 1): 9, (1, 2): 10, (2, 2): 11}
SECOND_ROLE = {-2: (0, 3, 2), -1: (3, 4, 1), 0: (7, 5, 0), 1: (12, 4, 0), 2: (16, 3, 0)}


def first_block(a, b):
    if a == 0:
        return 6 + b, False
    if b == 0:
        return 6 + a, True
    if (a, b) in FIRST_SLOT:
        return FIRST_SLOT[a, b], False
    return FIRST_SLOT[b, a], True


def second_block(a, b):
    return SECOND_ROLE[a][0] + b - max(-2, a - 2), False


def product(left, right, where):
    columns = []
    for b in range(-2, 3):
        total = None
        for a in range(max(-2, b - 2), min(2, b + 2) + 1):
            slot, flipped = where(a, b)
            term = lax.dot_general(
                left(a + 2),
                right[slot],
                (((1,), (1 if flipped else 0,)), ((), ())),
                preferred_element_type=jnp.float32,
            )
            total = term if total is None else total + term
        columns.append(total)
    return columns


def purify_kernel(
    density,
    kept,
    purified,
    first,
    second,
    squares,
    mine,
    final,
    kept_other,
    send_first,
    recv_first,
    send_pass,
    recv_pass,
    send_second,
    recv_second,
    send_pass_second,
    recv_pass_second,
    send_out,
    recv_out,
    kept_sems,
    own_sem,
):
    q = lax.axis_index("row")
    c = lax.axis_index("col")
    m = q // 2
    h = q % 2
    i = 8 * m + c
    rows = pl.ds(pl.multiple_of(HALF * h, HALF), HALF)
    sibling = dict(device_id={"row": 2 * m + 1 - h, "col": c}, device_id_type=pl.DeviceIdType.MESH)

    def chip(block_row):
        return dict(
            device_id={"row": 2 * (block_row // 8) + h, "col": block_row % 8},
            device_id_type=pl.DeviceIdType.MESH,
        )

    barrier = pltpu.get_barrier_semaphore()

    def greet(row, col):
        pl.semaphore_signal(
            barrier, inc=1, device_id={"row": row, "col": col}, device_id_type=pl.DeviceIdType.MESH
        )

    @pl.loop(0, COLS)
    def _(other):
        greet(2 * m + 1 - h, other)

        @pl.when(other != c)
        def _():
            greet(q, other)

        @pl.when((m > 0) & (((h == 0) & (other >= 6)) | ((h == 1) & (c <= 1))))
        def _():
            greet(q - 2, other)

        @pl.when((m < 7) & (((h == 1) & (other <= 1)) | ((h == 0) & (c >= 6))))
        def _():
            greet(q + 2, other)

    lower = jnp.where(m > 0, jnp.where(h == 0, 2, jnp.where(c <= 1, 8, 0)), 0)
    upper = jnp.where(m < 7, jnp.where(h == 1, 2, jnp.where(c >= 6, 8, 0)), 0)
    pl.semaphore_wait(barrier, 15 + lower + upper)

    kept_copy = pltpu.make_async_remote_copy(
        kept, kept_other, kept_sems.at[0], kept_sems.at[1], **sibling
    )
    kept_copy.start()

    def first_copies(local, act):
        k = 4 * q + local
        place = pl.ds(pl.multiple_of(SLICE * c, SLICE), SLICE)
        index = 0
        for role, pieces in FIRST_PIECES.items():
            target = k - role
            valid = (target >= 0) & (target < BLOCKS)
            for diagonal, count, slot in pieces:
                source = density.at[local, pl.ds(diagonal, count)]
                landing = first.at[pl.ds(slot, count), place]

                @pl.when(valid & (target != i))
                def _():
                    act(
                        pltpu.make_async_remote_copy(
                            source,
                            landing,
                            send_first.at[local, index],
                            recv_first.at[role + 2],
                            **chip(target),
                        ),
                        True,
                    )

                @pl.when(target == i)
                def _():
                    act(pltpu.make_async_copy(source, landing, recv_first.at[role + 2]), False)

                index += 1

    @pl.loop(0, 4)
    def _(local):
        first_copies(local, lambda copy, remote: copy.start())

    def pass_on(role):
        slot, count = FIRST_ROLE[role]
        part = first.at[pl.ds(slot, count)]
        return pltpu.make_async_remote_copy(
            part, part, send_pass.at[role + 2], recv_pass.at[role + 2], **sibling
        )

    order = (0, -1, 1, -2, 2)
    for role in order:
        slot, count = FIRST_ROLE[role]
        part = first.at[pl.ds(slot, count)]
        k = i + role
        valid = (k >= 0) & (k < BLOCKS)

        @pl.when(valid & ((k // 4) % 2 == h))
        def _():
            pltpu.make_async_copy(part, part, recv_first.at[role + 2]).wait()
            pass_on(role).start()

        @pl.when(jnp.logical_not(valid))
        def _():
            first[pl.ds(slot, count)] = jnp.zeros((count, WIDTH, WIDTH), jnp.bfloat16)
            start, number, _ = SECOND_ROLE[role]
            second[pl.ds(start, number)] = jnp.zeros((number, WIDTH, WIDTH), jnp.bfloat16)

    for role in order:
        k = i + role

        @pl.when((k >= 0) & (k < BLOCKS) & ((k // 4) % 2 != h))
        def _():
            pass_on(role).wait_recv()

    kept_copy.wait()
    near_kept = kept[c % 4]
    far_kept = kept_other[c % 4]
    mask = jnp.where(h == c // 4, near_kept, far_kept)

    def iterate(left, right, where, result):
        for d, total in enumerate(product(left, right, where)):
            squares[d] = jnp.where(mask[d : d + 1] > 0, total, 0.0).astype(jnp.bfloat16)
        for d, total in enumerate(product(lambda a: squares[a], right, where)):
            value = 3.0 * squares[d].astype(jnp.float32) - 2.0 * total
            result[d] = jnp.where(mask[d : d + 1] > 0, value, 0.0).astype(jnp.bfloat16)

    iterate(lambda a: first[4 + a, rows, :], first, first_block, mine)

    own = pltpu.make_async_copy(mine, second.at[pl.ds(7, 5), rows], own_sem)
    own.start()
    own_far = pltpu.make_async_remote_copy(
        mine, second.at[pl.ds(7, 5), rows], send_pass_second.at[2], recv_pass_second.at[2], **sibling
    )
    own_far.start()

    def second_copy(role):
        start, number, diagonal = SECOND_ROLE[role]
        return pltpu.make_async_remote_copy(
            mine.at[pl.ds(diagonal, number)],
            second.at[pl.ds(start, number), rows],
            send_second.at[role + 2],
            recv_second.at[role + 2],
            **chip(i - role),
        )

    def second_pass(role):
        start, number, _ = SECOND_ROLE[role]
        part = second.at[pl.ds(start, number), rows]
        return pltpu.make_async_remote_copy(
            part, part, send_pass_second.at[role + 2], recv_pass_second.at[role + 2], **sibling
        )

    others = (-2, 2, -1, 1)
    for role in others:
        target = i - role

        @pl.when((target >= 0) & (target < BLOCKS))
        def _():
            second_copy(role).start()

    for role in (-1, 1, -2, 2):
        k = i + role

        @pl.when((k >= 0) & (k < BLOCKS))
        def _():
            second_copy(role).wait_recv()
            second_pass(role).start()

    for role in (-1, 1, -2, 2):
        k = i + role

        @pl.when((k >= 0) & (k < BLOCKS))
        def _():
            second_pass(role).wait_recv()

    own.wait()
    own_far.wait_recv()
    iterate(lambda a: mine[a], second, second_block, final)

    def out_copies(act):
        for u in range(4):
            source = final.at[:, pl.ds(SLICE * u, SLICE)]
            landing = purified.at[c % 4]
            row, col = 2 * m + c // 4, 4 * h + u
            here = (row == q) & (col == c)

            @pl.when(jnp.logical_not(here))
            def _():
                act(
                    pltpu.make_async_remote_copy(
                        source,
                        landing,
                        send_out.at[u],
                        recv_out.at[c % 4],
                        device_id={"row": row, "col": col},
                        device_id_type=pl.DeviceIdType.MESH,
                    ),
                    True,
                )

            @pl.when(here)
            def _():
                act(pltpu.make_async_copy(source, landing, recv_out.at[c % 4]), False)

    out_copies(lambda copy, remote: copy.start())

    @pl.loop(0, 4)
    def _(local):
        first_copies(local, lambda copy, remote: copy.wait_send() if remote else None)

    for role in order:
        k = i + role

        @pl.when((k >= 0) & (k < BLOCKS) & ((k // 4) % 2 == h))
        def _():
            pass_on(role).wait_send()

    own_far.wait_send()
    for role in (-1, 1, -2, 2):
        target = i - role

        @pl.when((target >= 0) & (target < BLOCKS))
        def _():
            second_copy(role).wait_send()

        k = i + role

        @pl.when((k >= 0) & (k < BLOCKS))
        def _():
            second_pass(role).wait_send()

    out_copies(lambda copy, remote: copy.wait_send() if remote else None)
    for local in range(4):
        part = purified.at[local]
        pltpu.make_async_copy(part, part, recv_out.at[local]).wait()


def purify(density, pattern):
    blocks, diagonals, width, across = density.shape
    kept = jnp.broadcast_to(
        jnp.pad((pattern > 0).astype(jnp.float32), ((0, 0), (0, 3)))[:, :, None], (blocks, 8, WIDTH)
    )
    bf16, dma = jnp.bfloat16, pltpu.SemaphoreType.DMA
    vmem = pl.BlockSpec(memory_space=pltpu.VMEM)
    return pl.pallas_call(
        purify_kernel,
        name="purify",
        in_specs=[vmem, vmem],
        out_specs=vmem,
        out_shape=jax.ShapeDtypeStruct(density.shape, bf16),
        scratch_shapes=[
            pltpu.VMEM((12, WIDTH, WIDTH), bf16),
            pltpu.VMEM((19, WIDTH, WIDTH), bf16),
            pltpu.VMEM((BAND, HALF, WIDTH), bf16),
            pltpu.VMEM((BAND, HALF, WIDTH), bf16),
            pltpu.VMEM((BAND, HALF, WIDTH), bf16),
            pltpu.VMEM((4, 8, WIDTH), jnp.float32),
            dma((4, 6)),
            dma((5,)),
            dma((5,)),
            dma((5,)),
            dma((5,)),
            dma((5,)),
            dma((5,)),
            dma((5,)),
            dma((4,)),
            dma((4,)),
            dma((2,)),
            dma(()),
        ],
        compiler_params=pltpu.CompilerParams(
            collective_id=0, has_side_effects=True, vmem_limit_bytes=40 * 1024 * 1024
        ),
    )(density, kept)


def window_of(band_three, lead, offset, functions):
    paired = lax.dynamic_slice_in_dim(band_three, lead, 2, 0)
    upper = jnp.concatenate([paired[0, 1], paired[0, 2]], axis=1)
    lower = jnp.concatenate([paired[1, 0], paired[1, 1]], axis=1)
    dense = jnp.concatenate([upper, lower], axis=0)
    return lax.dynamic_slice(dense, (offset, offset), (functions, functions))


def spread_term(summed, term, lead, offset):
    width = summed.shape[2]
    dense = lax.dynamic_update_slice(
        jnp.zeros((2 * width, 2 * width), summed.dtype), term, (offset, offset)
    )
    nothing = jnp.zeros((width, width), summed.dtype)
    upper = jnp.stack([nothing, dense[:width, :width], dense[:width, width:]])
    lower = jnp.stack([dense[width:, :width], dense[width:, width:], nothing])
    increment = jnp.stack([upper, lower])
    paired = lax.dynamic_slice_in_dim(summed, lead, 2, 0)
    return lax.dynamic_update_slice_in_dim(summed, paired + increment, lead, 0)


def edge_rows(summed):
    blocks = summed.shape[0] - 2
    from_above = shifted_2(summed[0].astype(jnp.bfloat16), "row", -1).astype(jnp.float32)
    from_below = shifted_2(summed[blocks + 1].astype(jnp.bfloat16), "row", 1).astype(jnp.float32)
    own_rows = summed[1 : blocks + 1]
    return jnp.concatenate(
        [
            own_rows[:1] + from_below[None],
            own_rows[1 : blocks - 1],
            own_rows[blocks - 1 :] + from_above[None],
        ],
        axis=0,
    )


def on_device(density, pattern, windows, basis_values, basis_grads, weights):
    row_index = lax.axis_index("row")
    band_rows = density.shape[0]
    functions = basis_values.shape[2]
    step_size = functions // 3
    kept = (pattern > 0)[:, :, None, None]
    current = jnp.where(kept, density, jnp.zeros_like(density))
    current = purify(current, pattern)
    rows_band = gather_directly(current[:, 1:4], COL, 2)
    near = padded(rows_band, (("row", 0),), 1)
    tiles_here = windows.shape[0]
    block_size = near.shape[2]
    leads = [windows[t] // 2 - (band_rows * row_index - 1) for t in range(tiles_here)]
    offsets = [windows[t] % 2 * step_size for t in range(tiles_here)]
    window_blocks = jnp.stack(
        [window_of(near, leads[t], offsets[t], functions) for t in range(tiles_here)]
    )
    densities, contributions = tile_terms(basis_values, basis_grads, weights, window_blocks)
    local_terms = jnp.zeros((band_rows + 2, 3, block_size, block_size), jnp.float32)
    for t in range(tiles_here):
        local_terms = spread_term(local_terms, contributions[t], leads[t], offsets[t])
    owner_part = scatter_axes(local_terms.astype(jnp.bfloat16), (COL,), (0,), 2).astype(jnp.float32)
    mine = edge_rows(owner_part)
    xc_matrix = jnp.where(kept, jnp.pad(mine, ((0, 0), (1, 1), (0, 0), (0, 0))), 0.0)
    return (current, xc_matrix, densities)


def solution(mesh):
    placed = (
        P("row", None, COL, None),
        P("row", None),
        P(ROW_COL),
        P(ROW_COL, None, None),
        P(None, ROW_COL, None, None),
        P(ROW_COL, None),
    )
    return jax.shard_map(
        on_device,
        mesh=mesh,
        in_specs=placed,
        out_specs=(P("row", None, COL, None), P("row", None, COL, None), P(ROW_COL, None)),
        check_vma=False,
    )
```

```python
import jax
import jax.numpy as jnp
from jax import lax
from jax.experimental import pallas as pl
from jax.experimental.pallas import tpu as pltpu
from jax.sharding import PartitionSpec as P

COL = "col"
ROW_COL = ("row", "col")


slater_cx = 0.7386
kappa_pbe = 0.804
mu_pbe = 0.2195


POINT_BLOCK = 1024
CHUNK = 128


def potentials(density, grad_square):
    inverse_root = jnp.exp(jnp.log(density * density + 1.0) * (-1.0 / 3.0))
    inverse_two = inverse_root * inverse_root
    reduced = grad_square * (inverse_two * inverse_two)
    share = 1.0 / (1.0 + (mu_pbe / kappa_pbe) * reduced)
    enhance = 1.0 + kappa_pbe - kappa_pbe * share
    slope = mu_pbe * share * share
    by_density = (-slater_cx * 4.0 / 3.0) * inverse_root * density * (enhance - 2.0 * reduced * slope)
    by_gradient = -slater_cx * slope * inverse_two
    return by_density, by_gradient


def tile_kernel(
    starts, window_ref, values_ref, grads_ref, weights_ref, density_ref, term_ref, projected, weighted, total
):
    step = pl.program_id(1)
    functions = values_ref.shape[2]
    projected[...] = jnp.dot(values_ref[0], window_ref[0], preferred_element_type=jnp.float32)
    lane = lax.broadcasted_iota(jnp.int32, (8, 128), 1)
    packed = [jnp.zeros((8, 128), jnp.float32) for _ in range(4)]
    for chunk in range(POINT_BLOCK // CHUNK):
        rows = slice(chunk * CHUNK, (chunk + 1) * CHUNK)
        x = projected[rows, :]
        for k in range(4):
            basis = values_ref[0, rows, :] if k == 0 else grads_ref[k - 1, 0, rows, :]
            sums = jnp.sum(x * basis.astype(jnp.float32), axis=1, keepdims=True)
            for group in range(CHUNK // 8):
                here = chunk * (CHUNK // 8) + group
                packed[k] = jnp.where(lane == here, sums[8 * group : 8 * group + 8], packed[k])
    density = packed[0] / functions
    slopes = [2.0 * packed[k] / functions for k in (1, 2, 3)]
    grad_square = slopes[0] * slopes[0] + slopes[1] * slopes[1] + slopes[2] * slopes[2]
    by_density, by_gradient = potentials(density, grad_square)
    density_ref[0, 0] = density
    scaled = weights_ref[0, 0] * (1.0 / 4096.0)
    factors = [0.5 * by_density * scaled] + [2.0 * by_gradient * scaled * s for s in slopes]
    for pair in range(POINT_BLOCK // 16):
        rows = slice(pair * 16, pair * 16 + 16)
        z = None
        for k in range(4):
            basis = values_ref[0, rows, :] if k == 0 else grads_ref[k - 1, 0, rows, :]
            column = jnp.concatenate(
                [factors[k][:, 2 * pair : 2 * pair + 1], factors[k][:, 2 * pair + 1 : 2 * pair + 2]], axis=0
            )
            part = column * basis.astype(jnp.float32)
            z = part if z is None else z + part
        weighted[rows, :] = z.astype(jnp.bfloat16)
    one_side = lax.dot_general(
        values_ref[0], weighted[...], (((0,), (0,)), ((), ())), preferred_element_type=jnp.float32
    )

    @pl.when(step == 0)
    def _():
        total[...] = one_side

    @pl.when(step > 0)
    def _():
        total[...] += one_side

    @pl.when(step == pl.num_programs(1) - 1)
    def _():
        total[...] = total[...] + total[...].T
        shift = 4 * (starts[pl.program_id(0)] % 2)
        for holder in range(COLS):
            for which in range(2):
                piece = holder + 8 * which - shift
                inside = (piece >= 0) & (piece < 12)
                first_row = pl.multiple_of(SLICE * jnp.where(inside, piece, 0), SLICE)
                term_ref[holder, 0, which] = jnp.where(
                    inside, total[pl.ds(first_row, SLICE), :], 0.0
                ).astype(jnp.bfloat16)


def tile_terms(windows, values, grads, quadrature, window_blocks):
    tiles, points, functions = values.shape
    steps = points // POINT_BLOCK
    packed_weights = jnp.swapaxes(quadrature.reshape(tiles, steps, 128, 8), 2, 3)
    density, terms = pl.pallas_call(
        tile_kernel,
        name="tile_terms",
        grid=(tiles, steps),
        in_specs=[
            pl.BlockSpec(memory_space=pltpu.SMEM),
            pl.BlockSpec((1, functions, functions), lambda t, s: (t, 0, 0)),
            pl.BlockSpec((1, POINT_BLOCK, functions), lambda t, s: (t, s, 0)),
            pl.BlockSpec((3, 1, POINT_BLOCK, functions), lambda t, s: (0, t, s, 0)),
            pl.BlockSpec((1, 1, 8, 128), lambda t, s: (t, s, 0, 0)),
        ],
        out_specs=[
            pl.BlockSpec((1, 1, 8, 128), lambda t, s: (t, s, 0, 0)),
            pl.BlockSpec((COLS, 1, 2, SLICE, functions), lambda t, s: (0, t, 0, 0, 0)),
        ],
        out_shape=[
            jax.ShapeDtypeStruct((tiles, steps, 8, 128), jnp.float32),
            jax.ShapeDtypeStruct((COLS, tiles, 2, SLICE, functions), jnp.bfloat16),
        ],
        scratch_shapes=[
            pltpu.VMEM((POINT_BLOCK, functions), jnp.float32),
            pltpu.VMEM((POINT_BLOCK, functions), jnp.bfloat16),
            pltpu.VMEM((functions, functions), jnp.float32),
        ],
        compiler_params=pltpu.CompilerParams(
            dimension_semantics=("arbitrary", "arbitrary"), vmem_limit_bytes=40 * 1024 * 1024
        ),
        cost_estimate=pl.CostEstimate(
            flops=4 * tiles * points * functions * functions,
            bytes_accessed=8 * tiles * points * functions,
            transcendentals=0,
        ),
    )(windows, window_blocks, values, grads, packed_weights)
    return jnp.swapaxes(density, 2, 3).reshape(tiles, points), terms


BLOCKS = 64
BAND = 5
HALF = 128
WIDTH = 256
SLICE = 32
COLS = 8
FIRST_PIECES = {
    -2: ((2, 2, 0),),
    -1: ((2, 1, 2), (4, 1, 3)),
    0: ((0, 5, 4),),
    1: ((2, 2, 9),),
    2: ((2, 1, 11),),
}
FIRST_ROLE = {-2: (0, 2), -1: (2, 2), 0: (4, 5), 1: (9, 2), 2: (11, 1)}
FIRST_SLOT = {(-2, -2): 0, (-2, -1): 1, (-1, -1): 2, (-1, 1): 3, (1, 1): 9, (1, 2): 10, (2, 2): 11}
SECOND_ROLE = {-2: (0, 3, 2), -1: (3, 4, 1), 0: (7, 5, 0), 1: (12, 4, 0), 2: (16, 3, 0)}


def first_block(a, b):
    if a == 0:
        return 6 + b, False
    if b == 0:
        return 6 + a, True
    if (a, b) in FIRST_SLOT:
        return FIRST_SLOT[a, b], False
    return FIRST_SLOT[b, a], True


def second_block(a, b):
    return SECOND_ROLE[a][0] + b - max(-2, a - 2), False


def product(left, right, where):
    columns = []
    for b in range(-2, 3):
        total = None
        for a in range(max(-2, b - 2), min(2, b + 2) + 1):
            slot, flipped = where(a, b)
            term = lax.dot_general(
                left(a + 2),
                right[slot],
                (((1,), (1 if flipped else 0,)), ((), ())),
                preferred_element_type=jnp.float32,
            )
            total = term if total is None else total + term
        columns.append(total)
    return columns


def purify_kernel(
    density,
    kept,
    starts,
    purified,
    window_blocks,
    all_starts,
    first,
    second,
    squares,
    mine,
    final,
    kept_other,
    send_first,
    recv_first,
    send_pass,
    recv_pass,
    send_second,
    recv_second,
    send_pass_second,
    recv_pass_second,
    send_out,
    recv_out,
    kept_sems,
    own_sem,
    near,
    ready,
    staged,
    start_words,
    send_starts,
    recv_starts,
    send_edge,
    recv_edge,
    send_window,
    recv_window,
):
    q = lax.axis_index("row")
    c = lax.axis_index("col")
    m = q // 2
    h = q % 2
    i = 8 * m + c
    rows = pl.ds(pl.multiple_of(HALF * h, HALF), HALF)
    sibling = dict(device_id={"row": 2 * m + 1 - h, "col": c}, device_id_type=pl.DeviceIdType.MESH)

    def chip(block_row):
        return dict(
            device_id={"row": 2 * (block_row // 8) + h, "col": block_row % 8},
            device_id_type=pl.DeviceIdType.MESH,
        )

    barrier = pltpu.get_barrier_semaphore()

    def greet(row, col):
        pl.semaphore_signal(
            barrier, inc=1, device_id={"row": row, "col": col}, device_id_type=pl.DeviceIdType.MESH
        )

    @pl.loop(0, COLS)
    def _(other):
        greet(2 * m + 1 - h, other)

        @pl.when(other != c)
        def _():
            greet(q, other)

        @pl.when((m > 0) & (((h == 0) & (other >= 6)) | ((h == 1) & (c <= 1))))
        def _():
            greet(q - 2, other)

        @pl.when((m < 7) & (((h == 1) & (other <= 1)) | ((h == 0) & (c >= 6))))
        def _():
            greet(q + 2, other)

        @pl.when((m > 0) & (h == 0) & (((c == 0) & (other <= 3)) | ((c >= 4) & (other == 7))))
        def _():
            greet(q - 1, other)

        @pl.when((m < 7) & (h == 1) & (((c == 7) & (other >= 4)) | ((c <= 3) & (other == 0))))
        def _():
            greet(q + 1, other)

    lower = jnp.where(m > 0, jnp.where(h == 0, 2, jnp.where(c <= 1, 8, 0)), 0)
    upper = jnp.where(m < 7, jnp.where(h == 1, 2, jnp.where(c >= 6, 8, 0)), 0)
    lower_side = jnp.where((m > 0) & (h == 0), jnp.where(c == 0, 4, jnp.where(c >= 4, 1, 0)), 0)
    upper_side = jnp.where((m < 7) & (h == 1), jnp.where(c == 7, 4, jnp.where(c <= 3, 1, 0)), 0)
    pl.semaphore_wait(barrier, 15 + lower + upper + lower_side + upper_side)

    def start_copy(other):
        return pltpu.make_async_remote_copy(
            starts,
            all_starts.at[c],
            send_starts.at[other],
            recv_starts,
            device_id={"row": q, "col": other},
            device_id_type=pl.DeviceIdType.MESH,
        )

    @pl.loop(0, COLS)
    def _(other):
        @pl.when(other != c)
        def _():
            start_copy(other).start()

    pltpu.make_async_copy(starts, all_starts.at[c], recv_starts).start()

    kept_copy = pltpu.make_async_remote_copy(
        kept, kept_other, kept_sems.at[0], kept_sems.at[1], **sibling
    )
    kept_copy.start()

    def first_copies(local, act):
        k = 4 * q + local
        place = pl.ds(pl.multiple_of(SLICE * c, SLICE), SLICE)
        index = 0
        for role, pieces in FIRST_PIECES.items():
            target = k - role
            valid = (target >= 0) & (target < BLOCKS)
            for diagonal, count, slot in pieces:
                source = density.at[local, pl.ds(diagonal, count)]
                landing = first.at[pl.ds(slot, count), place]

                @pl.when(valid & (target != i))
                def _():
                    act(
                        pltpu.make_async_remote_copy(
                            source,
                            landing,
                            send_first.at[local, index],
                            recv_first.at[role + 2],
                            **chip(target),
                        ),
                        True,
                    )

                @pl.when(target == i)
                def _():
                    act(pltpu.make_async_copy(source, landing, recv_first.at[role + 2]), False)

                index += 1

    @pl.loop(0, 4)
    def _(local):
        first_copies(local, lambda copy, remote: copy.start())

    def pass_on(role):
        slot, count = FIRST_ROLE[role]
        part = first.at[pl.ds(slot, count)]
        return pltpu.make_async_remote_copy(
            part, part, send_pass.at[role + 2], recv_pass.at[role + 2], **sibling
        )

    order = (0, -1, 1, -2, 2)
    for role in order:
        slot, count = FIRST_ROLE[role]
        part = first.at[pl.ds(slot, count)]
        k = i + role
        valid = (k >= 0) & (k < BLOCKS)

        @pl.when(valid & ((k // 4) % 2 == h))
        def _():
            pltpu.make_async_copy(part, part, recv_first.at[role + 2]).wait()
            pass_on(role).start()

        @pl.when(jnp.logical_not(valid))
        def _():
            first[pl.ds(slot, count)] = jnp.zeros((count, WIDTH, WIDTH), jnp.bfloat16)
            start, number, _ = SECOND_ROLE[role]
            second[pl.ds(start, number)] = jnp.zeros((number, WIDTH, WIDTH), jnp.bfloat16)

    for role in order:
        k = i + role

        @pl.when((k >= 0) & (k < BLOCKS) & ((k // 4) % 2 != h))
        def _():
            pass_on(role).wait_recv()

    kept_copy.wait()
    near_kept = kept[c % 4]
    far_kept = kept_other[c % 4]
    mask = jnp.where(h == c // 4, near_kept, far_kept)

    def iterate(left, right, where, result):
        for d, total in enumerate(product(left, right, where)):
            squares[d] = jnp.where(mask[d : d + 1] > 0, total, 0.0).astype(jnp.bfloat16)
        for d, total in enumerate(product(lambda a: squares[a], right, where)):
            value = 3.0 * squares[d].astype(jnp.float32) - 2.0 * total
            result[d] = jnp.where(mask[d : d + 1] > 0, value, 0.0).astype(jnp.bfloat16)

    iterate(lambda a: first[4 + a, rows, :], first, first_block, mine)

    own = pltpu.make_async_copy(mine, second.at[pl.ds(7, 5), rows], own_sem)
    own.start()
    own_far = pltpu.make_async_remote_copy(
        mine, second.at[pl.ds(7, 5), rows], send_pass_second.at[2], recv_pass_second.at[2], **sibling
    )
    own_far.start()

    def second_copy(role):
        start, number, diagonal = SECOND_ROLE[role]
        return pltpu.make_async_remote_copy(
            mine.at[pl.ds(diagonal, number)],
            second.at[pl.ds(start, number), rows],
            send_second.at[role + 2],
            recv_second.at[role + 2],
            **chip(i - role),
        )

    def second_pass(role):
        start, number, _ = SECOND_ROLE[role]
        part = second.at[pl.ds(start, number), rows]
        return pltpu.make_async_remote_copy(
            part, part, send_pass_second.at[role + 2], recv_pass_second.at[role + 2], **sibling
        )

    others = (-2, 2, -1, 1)
    for role in others:
        target = i - role

        @pl.when((target >= 0) & (target < BLOCKS))
        def _():
            second_copy(role).start()

    for role in (-1, 1, -2, 2):
        k = i + role

        @pl.when((k >= 0) & (k < BLOCKS))
        def _():
            second_copy(role).wait_recv()
            second_pass(role).start()

    for role in (-1, 1, -2, 2):
        k = i + role

        @pl.when((k >= 0) & (k < BLOCKS))
        def _():
            second_pass(role).wait_recv()

    own.wait()
    own_far.wait_recv()
    iterate(lambda a: mine[a], second, second_block, final)

    def out_copies(act):
        for u in range(4):
            source = final.at[:, pl.ds(SLICE * u, SLICE)]
            landing = purified.at[c % 4]
            row, col = 2 * m + c // 4, 4 * h + u
            here = (row == q) & (col == c)

            @pl.when(jnp.logical_not(here))
            def _():
                act(
                    pltpu.make_async_remote_copy(
                        source,
                        landing,
                        send_out.at[u],
                        recv_out.at[c % 4],
                        device_id={"row": row, "col": col},
                        device_id_type=pl.DeviceIdType.MESH,
                    ),
                    True,
                )

            @pl.when(here)
            def _():
                act(pltpu.make_async_copy(source, landing, recv_out.at[c % 4]), False)

    def edge_copies(act):
        for side, reach, slot in ((0, -1, 5), (3, 1, 0)):
            row = 2 * m + c // 4 + reach

            @pl.when((c % 4 == side) & (row >= 0) & (row < 16))
            def _():
                for u in range(4):
                    here = (row == q) & (4 * h + u == c)
                    source = final.at[pl.ds(1, 3), pl.ds(SLICE * u, SLICE)]
                    landing = near.at[slot]
                    arrived = recv_edge.at[slot // 5]

                    @pl.when(jnp.logical_not(here))
                    def _():
                        act(
                            pltpu.make_async_remote_copy(
                                source,
                                landing,
                                send_edge.at[u],
                                arrived,
                                device_id={"row": row, "col": 4 * h + u},
                                device_id_type=pl.DeviceIdType.MESH,
                            ),
                            True,
                        )

                    @pl.when(here)
                    def _():
                        act(pltpu.make_async_copy(source, landing, arrived), False)

    edge_copies(lambda copy, remote: copy.start())
    out_copies(lambda copy, remote: copy.start())
    pltpu.make_async_copy(all_starts, all_starts, recv_starts).wait()
    words = pltpu.make_async_copy(all_starts, start_words, own_sem)
    words.start()
    words.wait()
    for local in range(4):
        part = purified.at[local]
        pltpu.make_async_copy(part, part, recv_out.at[local]).wait()
        near[local + 1] = purified[local, pl.ds(1, 3)]

    for side in range(2):
        part = near.at[5 * side]
        reached = (q < 15) if side else (q > 0)

        @pl.when(reached)
        def _():
            pltpu.make_async_copy(part, part, recv_edge.at[side]).wait()

        @pl.when(jnp.logical_not(reached))
        def _():
            near[5 * side] = jnp.zeros((3, SLICE, WIDTH), jnp.bfloat16)

    def window_copy(other):
        return pltpu.make_async_remote_copy(
            ready.at[other],
            staged.at[c],
            send_window.at[other],
            recv_window,
            device_id={"row": q, "col": other},
            device_id_type=pl.DeviceIdType.MESH,
        )

    @pl.loop(0, COLS)
    def _(other):
        for t in range(2):
            start = start_words[other, 0, t]
            lead = jnp.clip(start // 2 - (4 * q - 1), 0, 4)
            odd = (start % 2) == 1
            for which in range(2):
                left = near[lead + which, 1 - which]
                right = near[lead + which, 2 - which]
                for third, even_part, odd_part in (
                    (0, left[:, :128], left[:, 128:]),
                    (1, left[:, 128:], right[:, :128]),
                    (2, right[:, :128], right[:, 128:]),
                ):
                    ready[other, t, which, :, 128 * third : 128 * third + 128] = jnp.where(
                        odd, odd_part, even_part
                    )

        @pl.when(other != c)
        def _():
            window_copy(other).start()

        @pl.when(other == c)
        def _():
            pltpu.make_async_copy(ready.at[other], staged.at[c], recv_window).start()

    pltpu.make_async_copy(staged, staged, recv_window).wait()
    for t in range(2):
        shift = 4 * (start_words[c, 0, t] % 2)
        for u in range(12):
            at = shift + u
            window_blocks[t, SLICE * u : SLICE * u + SLICE, :] = staged[at % 8, t, at // 8]

    @pl.loop(0, 4)
    def _(local):
        first_copies(local, lambda copy, remote: copy.wait_send() if remote else None)

    for role in order:
        k = i + role

        @pl.when((k >= 0) & (k < BLOCKS) & ((k // 4) % 2 == h))
        def _():
            pass_on(role).wait_send()

    own_far.wait_send()
    for role in (-1, 1, -2, 2):
        target = i - role

        @pl.when((target >= 0) & (target < BLOCKS))
        def _():
            second_copy(role).wait_send()

        k = i + role

        @pl.when((k >= 0) & (k < BLOCKS))
        def _():
            second_pass(role).wait_send()

    out_copies(lambda copy, remote: copy.wait_send() if remote else None)
    edge_copies(lambda copy, remote: copy.wait_send() if remote else None)

    @pl.loop(0, COLS)
    def _(other):
        @pl.when(other != c)
        def _():
            start_copy(other).wait_send()
            window_copy(other).wait_send()


def purify(density, kept, windows):
    starts = jnp.broadcast_to(jnp.pad(windows, (0, 126))[None], (8, 128))
    functions = 3 * HALF
    bf16, dma = jnp.bfloat16, pltpu.SemaphoreType.DMA
    vmem = pl.BlockSpec(memory_space=pltpu.VMEM)
    return pl.pallas_call(
        purify_kernel,
        name="purify",
        in_specs=[vmem, vmem, vmem],
        out_specs=[vmem, vmem, vmem],
        out_shape=[
            jax.ShapeDtypeStruct(density.shape, bf16),
            jax.ShapeDtypeStruct((2, functions, functions), bf16),
            jax.ShapeDtypeStruct((COLS, 8, 128), jnp.int32),
        ],
        scratch_shapes=[
            pltpu.VMEM((12, WIDTH, WIDTH), bf16),
            pltpu.VMEM((19, WIDTH, WIDTH), bf16),
            pltpu.VMEM((BAND, HALF, WIDTH), bf16),
            pltpu.VMEM((BAND, HALF, WIDTH), bf16),
            pltpu.VMEM((BAND, HALF, WIDTH), bf16),
            pltpu.VMEM((4, 8, WIDTH), jnp.float32),
            dma((4, 6)),
            dma((5,)),
            dma((5,)),
            dma((5,)),
            dma((5,)),
            dma((5,)),
            dma((5,)),
            dma((5,)),
            dma((4,)),
            dma((4,)),
            dma((2,)),
            dma(()),
            pltpu.VMEM((6, 3, SLICE, WIDTH), bf16),
            pltpu.VMEM((COLS, 2, 2, SLICE, functions), bf16),
            pltpu.VMEM((COLS, 2, 2, SLICE, functions), bf16),
            pltpu.SMEM((COLS, 8, 128), jnp.int32),
            dma((COLS,)),
            dma(()),
            dma((4,)),
            dma((2,)),
            dma((COLS,)),
            dma(()),
        ],
        compiler_params=pltpu.CompilerParams(
            collective_id=0, has_side_effects=True, vmem_limit_bytes=40 * 1024 * 1024
        ),
    )(density, kept, starts)


def gather_terms_kernel(terms, kept, starts, matrix, staged, sums, edges, arrived, send, recv, send_edge, recv_edge):
    q = lax.axis_index("row")
    c = lax.axis_index("col")
    barrier = pltpu.get_barrier_semaphore()

    def greet(row, col):
        pl.semaphore_signal(
            barrier, inc=1, device_id={"row": row, "col": col}, device_id_type=pl.DeviceIdType.MESH
        )

    @pl.loop(0, COLS)
    def _(other):
        @pl.when(other != c)
        def _():
            greet(q, other)

    @pl.when(q > 0)
    def _():
        greet(q - 1, c)

    @pl.when(q < 15)
    def _():
        greet(q + 1, c)

    for s in range(COLS):
        for t in range(2):
            staged[s, t, 2] = jnp.zeros((SLICE, 3 * HALF), jnp.bfloat16)

    pl.semaphore_wait(barrier, 7 + jnp.where(q > 0, 1, 0) + jnp.where(q < 15, 1, 0))

    def term_copy(other):
        return pltpu.make_async_remote_copy(
            terms.at[other],
            staged.at[c, :, pl.ds(0, 2)],
            send.at[other],
            recv,
            device_id={"row": q, "col": other},
            device_id_type=pl.DeviceIdType.MESH,
        )

    @pl.loop(0, COLS)
    def _(other):
        @pl.when(other != c)
        def _():
            term_copy(other).start()

    pltpu.make_async_copy(terms.at[c], staged.at[c, :, pl.ds(0, 2)], recv).start()
    whole = staged.at[:, :, pl.ds(0, 2)]
    pltpu.make_async_copy(whole, whole, recv).wait()

    @pl.loop(0, 5)
    def _(lead):
        for which in range(2):
            for odd in range(2):
                total = None
                for s in range(COLS):
                    for t in range(2):
                        start = starts[2 * s + t]
                        chosen = (start // 2 - (4 * q - 1) == lead) & (start % 2 == odd)
                        piece = staged[s, t, jnp.where(chosen, which, 2)].astype(jnp.float32)
                        total = piece if total is None else total + piece
                sums[lead, which, odd] = total

    def block_row(r):
        wide = [jnp.zeros((SLICE, HALF), jnp.float32) for _ in range(6)]
        for which in range(2):
            if 0 <= r - which < 5:
                for odd in range(2):
                    piece = sums[r - which, which, odd]
                    for third in range(3):
                        place = 2 + odd - 2 * which + third
                        wide[place] = wide[place] + piece[:, HALF * third : HALF * third + HALF]
        return [jnp.concatenate(wide[2 * d : 2 * d + 2], axis=1) for d in range(3)]

    for side in range(2):
        for d, block in enumerate(block_row(5 * side)):
            edges[side, d] = block.astype(jnp.bfloat16)

    def edge_copy(side):
        return pltpu.make_async_remote_copy(
            edges.at[side],
            arrived.at[1 - side],
            send_edge.at[side],
            recv_edge.at[1 - side],
            device_id={"row": q + 2 * side - 1, "col": c},
            device_id_type=pl.DeviceIdType.MESH,
        )

    for side in range(2):
        reached = (q < 15) if side else (q > 0)

        @pl.when(reached)
        def _():
            edge_copy(side).start()

        @pl.when(jnp.logical_not(reached))
        def _():
            arrived[side] = jnp.zeros((3, SLICE, WIDTH), jnp.bfloat16)

    for local in (1, 2, 0, 3):
        if local in (0, 3):
            side = local // 3
            reached = (q < 15) if side else (q > 0)

            @pl.when(reached)
            def _():
                edge_copy(1 - side).wait_recv()

        blocks = block_row(local + 1)
        matrix[local, 0] = jnp.zeros((SLICE, WIDTH), jnp.float32)
        matrix[local, 4] = jnp.zeros((SLICE, WIDTH), jnp.float32)
        for d in range(3):
            block = blocks[d]
            if local in (0, 3):
                block = block + arrived[local // 3, d].astype(jnp.float32)
            matrix[local, d + 1] = jnp.where(kept[local, d + 1 : d + 2] > 0, block, 0.0)

    for side in range(2):
        reached = (q < 15) if side else (q > 0)

        @pl.when(reached)
        def _():
            edge_copy(side).wait_send()

    @pl.loop(0, COLS)
    def _(other):
        @pl.when(other != c)
        def _():
            term_copy(other).wait_send()


def gather_terms(terms, kept, starts):
    bf16, dma = jnp.bfloat16, pltpu.SemaphoreType.DMA
    vmem = pl.BlockSpec(memory_space=pltpu.VMEM)
    functions = 3 * HALF
    return pl.pallas_call(
        gather_terms_kernel,
        name="gather_terms",
        in_specs=[vmem, vmem, pl.BlockSpec(memory_space=pltpu.SMEM)],
        out_specs=vmem,
        out_shape=jax.ShapeDtypeStruct((4, BAND, SLICE, WIDTH), jnp.float32),
        scratch_shapes=[
            pltpu.VMEM((COLS, 2, 3, SLICE, functions), bf16),
            pltpu.VMEM((5, 2, 2, SLICE, functions), jnp.float32),
            pltpu.VMEM((2, 3, SLICE, WIDTH), bf16),
            pltpu.VMEM((2, 3, SLICE, WIDTH), bf16),
            dma((COLS,)),
            dma(()),
            dma((2,)),
            dma((2,)),
        ],
        compiler_params=pltpu.CompilerParams(
            collective_id=1, has_side_effects=True, vmem_limit_bytes=40 * 1024 * 1024
        ),
    )(terms, kept, starts)


def on_device(density, pattern, windows, basis_values, basis_grads, weights):
    band = (pattern > 0)[:, :, None, None]
    current = jnp.where(band, density, jnp.zeros_like(density))
    kept = jnp.broadcast_to(
        jnp.pad((pattern > 0).astype(jnp.float32), ((0, 0), (0, 3)))[:, :, None], (4, 8, WIDTH)
    )
    current, window_blocks, all_starts = purify(current, kept, windows)
    densities, terms = tile_terms(windows, basis_values, basis_grads, weights, window_blocks)
    xc_matrix = gather_terms(terms, kept, all_starts[:, 0, :2].reshape(-1))
    return (current, xc_matrix, densities)


def solution(mesh):
    placed = (
        P("row", None, COL, None),
        P("row", None),
        P(ROW_COL),
        P(ROW_COL, None, None),
        P(None, ROW_COL, None, None),
        P(ROW_COL, None),
    )
    return jax.shard_map(
        on_device,
        mesh=mesh,
        in_specs=placed,
        out_specs=(P("row", None, COL, None), P("row", None, COL, None), P(ROW_COL, None)),
        check_vma=False,
    )
```

```python
import jax
import jax.numpy as jnp
from jax import lax
from jax.experimental import pallas as pl
from jax.experimental.pallas import tpu as pltpu
from jax.sharding import PartitionSpec as P

COL = "col"
ROW_COL = ("row", "col")


slater_cx = 0.7386
kappa_pbe = 0.804
mu_pbe = 0.2195


POINT_BLOCK = 1024
STEPS = 4
LANES = 256
FUNCTIONS = 384


def potentials(density, grad_square):
    inverse_root = jnp.exp(jnp.log(density * density + 1.0) * (-1.0 / 3.0))
    inverse_two = inverse_root * inverse_root
    reduced = grad_square * (inverse_two * inverse_two)
    share = 1.0 / (1.0 + (mu_pbe / kappa_pbe) * reduced)
    enhance = 1.0 + kappa_pbe - kappa_pbe * share
    slope = mu_pbe * share * share
    by_density = (-slater_cx * 4.0 / 3.0) * inverse_root * density * (enhance - 2.0 * reduced * slope)
    by_gradient = -slater_cx * slope * inverse_two
    return by_density, by_gradient


BLOCKS = 64
BAND = 5
HALF = 128
WIDTH = 256
SLICE = 32
COLS = 8
FIRST_PIECES = {
    -2: ((2, 2, 0),),
    -1: ((2, 1, 2), (4, 1, 3)),
    0: ((0, 5, 4),),
    1: ((2, 2, 9),),
    2: ((2, 1, 11),),
}
FIRST_ROLE = {-2: (0, 2), -1: (2, 2), 0: (4, 5), 1: (9, 2), 2: (11, 1)}
FIRST_SLOT = {(-2, -2): 0, (-2, -1): 1, (-1, -1): 2, (-1, 1): 3, (1, 1): 9, (1, 2): 10, (2, 2): 11}
SECOND_ROLE = {-2: (0, 3, 2), -1: (3, 4, 1), 0: (7, 5, 0), 1: (12, 4, 0), 2: (16, 3, 0)}


def first_block(a, b):
    if a == 0:
        return 6 + b, False
    if b == 0:
        return 6 + a, True
    if (a, b) in FIRST_SLOT:
        return FIRST_SLOT[a, b], False
    return FIRST_SLOT[b, a], True


def second_block(a, b):
    return SECOND_ROLE[a][0] + b - max(-2, a - 2), False


def product(left, right, where):
    columns = []
    for b in range(-2, 3):
        total = None
        for a in range(max(-2, b - 2), min(2, b + 2) + 1):
            slot, flipped = where(a, b)
            term = lax.dot_general(
                left(a + 2),
                right[slot],
                (((1,), (1 if flipped else 0,)), ((), ())),
                preferred_element_type=jnp.float32,
            )
            total = term if total is None else total + term
        columns.append(total)
    return columns


def fused_kernel(
    density,
    pattern,
    windows,
    values,
    grads,
    weights,
    purified,
    matrix,
    densities,
    masked,
    kept,
    kept_other,
    starts,
    all_starts,
    start_words,
    natural,
    turned,
    first,
    second,
    squares,
    mine,
    final,
    near,
    ready,
    staged_first,
    staged_second,
    window,
    projected,
    weighted,
    total,
    rows_of,
    terms,
    gathered_first,
    gathered_second,
    sums,
    edges,
    arrived,
    load_sems,
    kept_sems,
    send_starts,
    recv_starts,
    send_first,
    recv_first,
    send_pass,
    recv_pass,
    send_second,
    recv_second,
    send_pass_second,
    recv_pass_second,
    own_sem,
    send_out,
    recv_out,
    send_edge,
    recv_edge,
    send_window,
    recv_window,
    send_terms,
    recv_terms,
    send_sum,
    recv_sum,
):
    staged, gathered = (staged_first, staged_second), (gathered_first, gathered_second)
    q = lax.axis_index("row")
    c = lax.axis_index("col")
    m = q // 2
    h = q % 2
    j = 2 * (c % 4) + c // 4
    i = 8 * m + j
    rows = pl.ds(pl.multiple_of(HALF * h, HALF), HALF)
    sibling = dict(device_id={"row": 2 * m + 1 - h, "col": c}, device_id_type=pl.DeviceIdType.MESH)

    def chip(block_row):
        return dict(
            device_id={"row": 2 * (block_row // 8) + h, "col": block_row % 2 * 4 + block_row % 8 // 2},
            device_id_type=pl.DeviceIdType.MESH,
        )

    def load(n):
        slot = n % 2
        tile, part = n // STEPS, pl.ds(pl.multiple_of(n % STEPS * POINT_BLOCK, POINT_BLOCK), POINT_BLOCK)
        return (
            pltpu.make_async_copy(values.at[tile, part], natural.at[slot, 0], load_sems.at[slot, 0]),
            pltpu.make_async_copy(grads.at[:, tile, part], natural.at[slot, pl.ds(1, 3)], load_sems.at[slot, 1]),
        )

    for n in range(2):
        for copy in load(n):
            copy.start()

    barrier = pltpu.get_barrier_semaphore()

    def greet(row, col):
        pl.semaphore_signal(
            barrier, inc=1, device_id={"row": row, "col": col}, device_id_type=pl.DeviceIdType.MESH
        )

    @pl.loop(0, COLS)
    def _(other):
        greet(2 * m + 1 - h, other)

        @pl.when(other != c)
        def _():
            greet(q, other)

        @pl.when((m > 0) & (((h == 0) & (other % 4 == 3)) | ((h == 1) & (c % 4 == 0))))
        def _():
            greet(q - 2, other)

        @pl.when((m < 7) & (((h == 1) & (other % 4 == 0)) | ((h == 0) & (c % 4 == 3))))
        def _():
            greet(q + 2, other)

        @pl.when((m > 0) & (h == 0) & (((c == 0) & (other <= 3)) | ((c >= 4) & (other == 7)) | (other == c)))
        def _():
            greet(q - 1, other)

        @pl.when((m < 7) & (h == 1) & (((c == 7) & (other >= 4)) | ((c <= 3) & (other == 0)) | (other == c)))
        def _():
            greet(q + 1, other)

    lower = jnp.where(m > 0, jnp.where(h == 0, 2, jnp.where(c % 4 == 0, 8, 0)), 0)
    upper = jnp.where(m < 7, jnp.where(h == 1, 2, jnp.where(c % 4 == 3, 8, 0)), 0)
    some = jnp.where((c >= 4) & (c <= 6), 2, 1)
    lower_side = jnp.where((m > 0) & (h == 0), jnp.where(c == 0, 4, some), 0)
    some = jnp.where((c >= 1) & (c <= 3), 2, 1)
    upper_side = jnp.where((m < 7) & (h == 1), jnp.where(c == 7, 4, some), 0)

    for local in range(4):
        for d in range(BAND):
            flag = pattern[local, d] > 0
            masked[local, d] = jnp.where(flag, density[local, d], jnp.zeros((SLICE, WIDTH), jnp.bfloat16))
            kept[local, d : d + 1] = jnp.where(flag, jnp.ones((1, WIDTH), jnp.float32), 0.0)
    lane = lax.broadcasted_iota(jnp.int32, (8, 128), 1)
    starts[...] = jnp.where(lane == 0, windows[0], windows[1])
    pl.semaphore_wait(barrier, 15 + lower + upper + lower_side + upper_side)

    def start_copy(other):
        return pltpu.make_async_remote_copy(
            starts,
            all_starts.at[c],
            send_starts.at[other],
            recv_starts,
            device_id={"row": q, "col": other},
            device_id_type=pl.DeviceIdType.MESH,
        )

    @pl.loop(0, COLS)
    def _(other):
        @pl.when(other != c)
        def _():
            start_copy(other).start()

    pltpu.make_async_copy(starts, all_starts.at[c], recv_starts).start()

    kept_copy = pltpu.make_async_remote_copy(
        kept, kept_other, kept_sems.at[0], kept_sems.at[1], **sibling
    )
    kept_copy.start()

    def first_copies(local, act):
        k = 4 * q + local
        place = pl.ds(pl.multiple_of(SLICE * c, SLICE), SLICE)
        index = 0
        for role, pieces in FIRST_PIECES.items():
            target = k - role
            valid = (target >= 0) & (target < BLOCKS)
            for diagonal, count, slot in pieces:
                source = masked.at[local, pl.ds(diagonal, count)]
                landing = first.at[pl.ds(slot, count), place]

                @pl.when(valid & (target != i))
                def _():
                    act(
                        pltpu.make_async_remote_copy(
                            source,
                            landing,
                            send_first.at[local, index],
                            recv_first.at[role + 2],
                            **chip(target),
                        ),
                        True,
                    )

                @pl.when(target == i)
                def _():
                    act(pltpu.make_async_copy(source, landing, recv_first.at[role + 2]), False)

                index += 1

    @pl.loop(0, 4)
    def _(local):
        first_copies(local, lambda copy, remote: copy.start())

    @pl.loop(0, 2 * STEPS)
    def _(n):
        for copy in load(n):
            copy.wait()
        for k in range(4):
            turned[n, k] = natural[n % 2, k].T

        @pl.when(n < 2 * STEPS - 2)
        def _():
            for copy in load(n + 2):
                copy.start()

    def pass_on(role):
        slot, count = FIRST_ROLE[role]
        part = first.at[pl.ds(slot, count)]
        return pltpu.make_async_remote_copy(
            part, part, send_pass.at[role + 2], recv_pass.at[role + 2], **sibling
        )

    order = (0, -1, 1, -2, 2)
    for role in order:
        slot, count = FIRST_ROLE[role]
        part = first.at[pl.ds(slot, count)]
        k = i + role
        valid = (k >= 0) & (k < BLOCKS)

        @pl.when(valid & ((k // 4) % 2 == h))
        def _():
            pltpu.make_async_copy(part, part, recv_first.at[role + 2]).wait()
            pass_on(role).start()

        @pl.when(jnp.logical_not(valid))
        def _():
            first[pl.ds(slot, count)] = jnp.zeros((count, WIDTH, WIDTH), jnp.bfloat16)
            start, number, _ = SECOND_ROLE[role]
            second[pl.ds(start, number)] = jnp.zeros((number, WIDTH, WIDTH), jnp.bfloat16)

    for role in order:
        k = i + role

        @pl.when((k >= 0) & (k < BLOCKS) & ((k // 4) % 2 != h))
        def _():
            pass_on(role).wait_recv()

    kept_copy.wait()
    near_kept = kept[j % 4]
    far_kept = kept_other[j % 4]
    mask = jnp.where(h == j // 4, near_kept, far_kept)

    def iterate(left, right, where, result):
        for d, total in enumerate(product(left, right, where)):
            squares[d] = jnp.where(mask[d : d + 1] > 0, total, 0.0).astype(jnp.bfloat16)
        for d, total in enumerate(product(lambda a: squares[a], right, where)):
            value = 3.0 * squares[d].astype(jnp.float32) - 2.0 * total
            result[d] = jnp.where(mask[d : d + 1] > 0, value, 0.0).astype(jnp.bfloat16)

    iterate(lambda a: first[4 + a, rows, :], first, first_block, mine)

    own = pltpu.make_async_copy(mine, second.at[pl.ds(7, 5), rows], own_sem)
    own.start()
    own_far = pltpu.make_async_remote_copy(
        mine, second.at[pl.ds(7, 5), rows], send_pass_second.at[2], recv_pass_second.at[2], **sibling
    )
    own_far.start()

    def second_copy(role):
        start, number, diagonal = SECOND_ROLE[role]
        return pltpu.make_async_remote_copy(
            mine.at[pl.ds(diagonal, number)],
            second.at[pl.ds(start, number), rows],
            send_second.at[role + 2],
            recv_second.at[role + 2],
            **chip(i - role),
        )

    def second_pass(role):
        start, number, _ = SECOND_ROLE[role]
        part = second.at[pl.ds(start, number), rows]
        return pltpu.make_async_remote_copy(
            part, part, send_pass_second.at[role + 2], recv_pass_second.at[role + 2], **sibling
        )

    others = (-2, 2, -1, 1)
    for role in others:
        target = i - role

        @pl.when((target >= 0) & (target < BLOCKS))
        def _():
            second_copy(role).start()

    for role in (-1, 1, -2, 2):
        k = i + role

        @pl.when((k >= 0) & (k < BLOCKS))
        def _():
            second_copy(role).wait_recv()
            second_pass(role).start()

    for role in (-1, 1, -2, 2):
        k = i + role

        @pl.when((k >= 0) & (k < BLOCKS))
        def _():
            second_pass(role).wait_recv()

    own.wait()
    own_far.wait_recv()
    iterate(lambda a: mine[a], second, second_block, final)

    def out_copies(part, act):
        diagonal, count = ((1, 3), (0, 1), (4, 1))[part]
        for u in range(4):
            source = final.at[pl.ds(diagonal, count), pl.ds(SLICE * u, SLICE)]
            landing = purified.at[j % 4, pl.ds(diagonal, count)]
            row, col = 2 * m + j // 4, 4 * h + u
            here = (row == q) & (col == c)

            @pl.when(jnp.logical_not(here))
            def _():
                act(
                    pltpu.make_async_remote_copy(
                        source,
                        landing,
                        send_out.at[part, u],
                        recv_out.at[part, j % 4],
                        device_id={"row": row, "col": col},
                        device_id_type=pl.DeviceIdType.MESH,
                    ),
                    True,
                )

            @pl.when(here)
            def _():
                act(pltpu.make_async_copy(source, landing, recv_out.at[part, j % 4]), False)

    def edge_copies(act):
        for side, reach, slot in ((0, -1, 5), (3, 1, 0)):
            row = 2 * m + j // 4 + reach

            @pl.when((j % 4 == side) & (row >= 0) & (row < 16))
            def _():
                for u in range(4):
                    here = (row == q) & (4 * h + u == c)
                    source = final.at[pl.ds(1, 3), pl.ds(SLICE * u, SLICE)]
                    landing = near.at[slot]
                    arrived = recv_edge.at[slot // 5]

                    @pl.when(jnp.logical_not(here))
                    def _():
                        act(
                            pltpu.make_async_remote_copy(
                                source,
                                landing,
                                send_edge.at[u],
                                arrived,
                                device_id={"row": row, "col": 4 * h + u},
                                device_id_type=pl.DeviceIdType.MESH,
                            ),
                            True,
                        )

                    @pl.when(here)
                    def _():
                        act(pltpu.make_async_copy(source, landing, arrived), False)

    edge_copies(lambda copy, remote: copy.start())
    out_copies(0, lambda copy, remote: copy.start())
    pltpu.make_async_copy(all_starts, all_starts, recv_starts).wait()
    words = pltpu.make_async_copy(all_starts, start_words, own_sem)
    words.start()
    words.wait()
    for local in range(4):
        part = purified.at[local, pl.ds(1, 3)]
        pltpu.make_async_copy(part, part, recv_out.at[0, local]).wait()
        near[local + 1] = purified[local, pl.ds(1, 3)]

    for side in range(2):
        part = near.at[5 * side]
        reached = (q < 15) if side else (q > 0)

        @pl.when(reached)
        def _():
            pltpu.make_async_copy(part, part, recv_edge.at[side]).wait()

        @pl.when(jnp.logical_not(reached))
        def _():
            near[5 * side] = jnp.zeros((3, SLICE, WIDTH), jnp.bfloat16)

    def window_copy(other, t):
        return pltpu.make_async_remote_copy(
            ready.at[other, t],
            staged[t].at[c],
            send_window.at[other, t],
            recv_window.at[t],
            device_id={"row": q, "col": other},
            device_id_type=pl.DeviceIdType.MESH,
        )

    for t in range(2):

        @pl.loop(1, COLS + 1)
        def _(step):
            other = (c + step) % COLS
            start = start_words[other, 0, t]
            lead = jnp.clip(start // 2 - (4 * q - 1), 0, 4)
            odd = (start % 2) == 1
            for which in range(2):
                left = near[lead + which, 1 - which]
                right = near[lead + which, 2 - which]
                for third, even_part, odd_part in (
                    (0, left[:, :128], left[:, 128:]),
                    (1, left[:, 128:], right[:, :128]),
                    (2, right[:, :128], right[:, 128:]),
                ):
                    ready[other, t, which, :, 128 * third : 128 * third + 128] = jnp.where(
                        odd, odd_part, even_part
                    )

            @pl.when(other != c)
            def _():
                window_copy(other, t).start()

            @pl.when(other == c)
            def _():
                pltpu.make_async_copy(ready.at[other, t], staged[t].at[c], recv_window.at[t]).start()

    for part in (1, 2):
        out_copies(part, lambda copy, remote: copy.start())

    def term_copy(other, t):
        return pltpu.make_async_remote_copy(
            terms.at[other, t],
            gathered[t].at[c, pl.ds(0, 2)],
            send_terms.at[other, t],
            recv_terms.at[t],
            device_id={"row": q, "col": other},
            device_id_type=pl.DeviceIdType.MESH,
        )

    for s in range(COLS):
        for t in range(2):
            gathered[t][s, 2] = jnp.zeros((SLICE, FUNCTIONS), jnp.bfloat16)

    rows_of[12] = jnp.zeros((SLICE, FUNCTIONS), jnp.bfloat16)

    for t in range(2):
        part = staged[t]
        pltpu.make_async_copy(part, part, recv_window.at[t]).wait()
        shift = 4 * (start_words[c, 0, t] % 2)
        for u in range(12):
            at = shift + u
            window[SLICE * u : SLICE * u + SLICE, :] = staged[t][at % 8, at // 8]
        window[...] = window[...].T
        total[...] = jnp.zeros_like(total)
        weighted[1] = jnp.zeros((FUNCTIONS, POINT_BLOCK), jnp.bfloat16)
        projected[0] = jnp.dot(window[...], turned[STEPS * t, 0], preferred_element_type=jnp.float32)

        @pl.loop(0, STEPS)
        def _(s):
            n = STEPS * t + s
            now, later = s % 2, (s + 1) % 2
            ahead = STEPS * t + jnp.minimum(s + 1, STEPS - 1)
            behind = STEPS * t + jnp.maximum(s - 1, 0)
            projected[later] = jnp.dot(window[...], turned[ahead, 0], preferred_element_type=jnp.float32)
            total[...] += lax.dot_general(
                turned[behind, 0], weighted[later], (((1,), (1,)), ((), ())), preferred_element_type=jnp.float32
            )
            for piece in range(POINT_BLOCK // LANES):
                lanes = slice(piece * LANES, piece * LANES + LANES)
                points = pl.ds(pl.multiple_of(s * POINT_BLOCK + piece * LANES, LANES), LANES)
                x = projected[now, :, lanes]
                reduced = [
                    jnp.sum(x * turned[n, k, :, lanes].astype(jnp.float32), axis=0, keepdims=True)
                    for k in range(4)
                ]
                point_density = reduced[0] / FUNCTIONS
                slopes = [2.0 * r / FUNCTIONS for r in reduced[1:]]
                grad_square = slopes[0] * slopes[0] + slopes[1] * slopes[1] + slopes[2] * slopes[2]
                by_density, by_gradient = potentials(point_density, grad_square)
                densities[t : t + 1, points] = point_density
                scaled = weights[t : t + 1, points] * (1.0 / 4096.0)
                factors = [0.5 * by_density * scaled] + [2.0 * by_gradient * scaled * s for s in slopes]
                z = None
                for k in range(4):
                    factor = jnp.broadcast_to(factors[k], (16, LANES)).astype(jnp.bfloat16)
                    basis = turned[n, k, :, lanes].reshape(FUNCTIONS // 16, 16, LANES)
                    z = factor[None] * basis if z is None else z + factor[None] * basis
                weighted[now, :, lanes] = z.reshape(FUNCTIONS, LANES)

        total[...] += lax.dot_general(
            turned[STEPS * t + STEPS - 1, 0],
            weighted[(STEPS - 1) % 2],
            (((1,), (1,)), ((), ())),
            preferred_element_type=jnp.float32,
        )
        both = total[...] + total[...].T
        for piece in range(12):
            rows_of[piece] = both[SLICE * piece : SLICE * piece + SLICE].astype(jnp.bfloat16)

        @pl.loop(1, COLS + 1)
        def _(step):
            holder = (c + step) % COLS
            for which in range(2):
                piece = holder + 8 * which - shift
                inside = (piece >= 0) & (piece < 12)
                terms[holder, t, which] = rows_of[jnp.where(inside, piece, 12)]

            @pl.when(holder != c)
            def _():
                term_copy(holder, t).start()

            @pl.when(holder == c)
            def _():
                pltpu.make_async_copy(
                    terms.at[holder, t], gathered[t].at[c, pl.ds(0, 2)], recv_terms.at[t]
                ).start()

    def sum_copy(side):
        return pltpu.make_async_remote_copy(
            edges.at[side],
            arrived.at[1 - side],
            send_sum.at[side],
            recv_sum.at[1 - side],
            device_id={"row": q + 2 * side - 1, "col": c},
            device_id_type=pl.DeviceIdType.MESH,
        )

    def add_up(t, lead, which):
        for odd in range(2):
            together = None if t == 0 else sums[lead, which, odd]
            for s in range(COLS):
                start = start_words[s, 0, t]
                chosen = (start // 2 - (4 * q - 1) == lead) & (start % 2 == odd)
                piece = gathered[t][s, jnp.where(chosen, which, 2)].astype(jnp.float32)
                together = piece if together is None else together + piece
            sums[lead, which, odd] = together

    def block_row(r):
        wide = [jnp.zeros((SLICE, HALF), jnp.float32) for _ in range(6)]
        for which in range(2):
            if 0 <= r - which < 5:
                for odd in range(2):
                    piece = sums[r - which, which, odd]
                    for third in range(3):
                        place = 2 + odd - 2 * which + third
                        wide[place] = wide[place] + piece[:, HALF * third : HALF * third + HALF]
        return [jnp.concatenate(wide[2 * d : 2 * d + 2], axis=1) for d in range(3)]

    for t in range(2):
        part = gathered[t].at[:, pl.ds(0, 2)]
        pltpu.make_async_copy(part, part, recv_terms.at[t]).wait()
        add_up(t, 0, 0)
        add_up(t, 4, 1)
        if t == 1:
            for side in range(2):
                for d, block in enumerate(block_row(5 * side)):
                    edges[side, d] = block.astype(jnp.bfloat16)
                reached = (q < 15) if side else (q > 0)

                @pl.when(reached)
                def _():
                    sum_copy(side).start()

        @pl.loop(0, 4)
        def _(lead):
            add_up(t, lead + 1, 0)
            add_up(t, lead, 1)

    for side in range(2):
        reached = (q < 15) if side else (q > 0)

        @pl.when(jnp.logical_not(reached))
        def _():
            arrived[side] = jnp.zeros((3, SLICE, WIDTH), jnp.bfloat16)

    for local in (1, 2, 0, 3):
        if local in (0, 3):
            side = local // 3
            reached = (q < 15) if side else (q > 0)

            @pl.when(reached)
            def _():
                sum_copy(1 - side).wait_recv()

        blocks = block_row(local + 1)
        matrix[local, 0] = jnp.zeros((SLICE, WIDTH), jnp.float32)
        matrix[local, 4] = jnp.zeros((SLICE, WIDTH), jnp.float32)
        for d in range(3):
            block = blocks[d]
            if local in (0, 3):
                block = block + arrived[local // 3, d].astype(jnp.float32)
            matrix[local, d + 1] = jnp.where(pattern[local, d + 1] > 0, block, 0.0)

    for side in range(2):
        reached = (q < 15) if side else (q > 0)

        @pl.when(reached)
        def _():
            sum_copy(side).wait_send()

    @pl.loop(0, 4)
    def _(local):
        first_copies(local, lambda copy, remote: copy.wait_send() if remote else None)

    for role in order:
        k = i + role

        @pl.when((k >= 0) & (k < BLOCKS) & ((k // 4) % 2 == h))
        def _():
            pass_on(role).wait_send()

    own_far.wait_send()
    for role in (-1, 1, -2, 2):
        target = i - role

        @pl.when((target >= 0) & (target < BLOCKS))
        def _():
            second_copy(role).wait_send()

        k = i + role

        @pl.when((k >= 0) & (k < BLOCKS))
        def _():
            second_pass(role).wait_send()

    for part in range(3):
        out_copies(part, lambda copy, remote: copy.wait_send() if remote else None)
    for part, diagonal in ((1, 0), (2, 4)):
        for local in range(4):
            block = purified.at[local, pl.ds(diagonal, 1)]
            pltpu.make_async_copy(block, block, recv_out.at[part, local]).wait()
    edge_copies(lambda copy, remote: copy.wait_send() if remote else None)

    @pl.loop(0, COLS)
    def _(other):
        @pl.when(other != c)
        def _():
            start_copy(other).wait_send()
            for t in range(2):
                window_copy(other, t).wait_send()
                term_copy(other, t).wait_send()


def on_device(density, pattern, windows, basis_values, basis_grads, weights):
    bf16, f32, dma = jnp.bfloat16, jnp.float32, pltpu.SemaphoreType.DMA
    vmem = pl.BlockSpec(memory_space=pltpu.VMEM)
    smem = pl.BlockSpec(memory_space=pltpu.SMEM)
    hbm = pl.BlockSpec(memory_space=pl.ANY)
    half_row = pltpu.VMEM((BAND, HALF, WIDTH), bf16)
    pieces = pltpu.VMEM((COLS, 2, 2, SLICE, FUNCTIONS), bf16)
    edge = pltpu.VMEM((2, 3, SLICE, WIDTH), bf16)
    return pl.pallas_call(
        fused_kernel,
        name="fused",
        in_specs=[vmem, smem, smem, hbm, hbm, vmem],
        out_specs=[vmem, vmem, vmem],
        out_shape=[
            jax.ShapeDtypeStruct(density.shape, bf16),
            jax.ShapeDtypeStruct(density.shape, f32),
            jax.ShapeDtypeStruct(weights.shape, f32),
        ],
        scratch_shapes=[
            pltpu.VMEM(density.shape, bf16),
            pltpu.VMEM((4, 8, WIDTH), f32),
            pltpu.VMEM((4, 8, WIDTH), f32),
            pltpu.VMEM((8, 128), jnp.int32),
            pltpu.VMEM((COLS, 8, 128), jnp.int32),
            pltpu.SMEM((COLS, 8, 128), jnp.int32),
            pltpu.VMEM((2, 4, POINT_BLOCK, FUNCTIONS), bf16),
            pltpu.VMEM((2 * STEPS, 4, FUNCTIONS, POINT_BLOCK), bf16),
            pltpu.VMEM((12, WIDTH, WIDTH), bf16),
            pltpu.VMEM((19, WIDTH, WIDTH), bf16),
            half_row,
            half_row,
            half_row,
            pltpu.VMEM((6, 3, SLICE, WIDTH), bf16),
            pieces,
            pltpu.VMEM((COLS, 2, SLICE, FUNCTIONS), bf16),
            pltpu.VMEM((COLS, 2, SLICE, FUNCTIONS), bf16),
            pltpu.VMEM((FUNCTIONS, FUNCTIONS), bf16),
            pltpu.VMEM((2, FUNCTIONS, POINT_BLOCK), f32),
            pltpu.VMEM((2, FUNCTIONS, POINT_BLOCK), bf16),
            pltpu.VMEM((FUNCTIONS, FUNCTIONS), f32),
            pltpu.VMEM((13, SLICE, FUNCTIONS), bf16),
            pieces,
            pltpu.VMEM((COLS, 3, SLICE, FUNCTIONS), bf16),
            pltpu.VMEM((COLS, 3, SLICE, FUNCTIONS), bf16),
            pltpu.VMEM((5, 2, 2, SLICE, FUNCTIONS), f32),
            edge,
            edge,
            dma((2, 2)),
            dma((2,)),
            dma((COLS,)),
            dma(()),
            dma((4, 6)),
            dma((5,)),
            dma((5,)),
            dma((5,)),
            dma((5,)),
            dma((5,)),
            dma((5,)),
            dma((5,)),
            dma(()),
            dma((3, 4)),
            dma((3, 4)),
            dma((4,)),
            dma((2,)),
            dma((COLS, 2)),
            dma((2,)),
            dma((COLS, 2)),
            dma((2,)),
            dma((2,)),
            dma((2,)),
        ],
        compiler_params=pltpu.CompilerParams(
            collective_id=0, has_side_effects=True, vmem_limit_bytes=63 * 1024 * 1024
        ),
    )(density, pattern, windows, basis_values, basis_grads, weights)


def solution(mesh):
    placed = (
        P("row", None, COL, None),
        P("row", None),
        P(ROW_COL),
        P(ROW_COL, None, None),
        P(None, ROW_COL, None, None),
        P(ROW_COL, None),
    )
    return jax.shard_map(
        on_device,
        mesh=mesh,
        in_specs=placed,
        out_specs=(P("row", None, COL, None), P("row", None, COL, None), P(ROW_COL, None)),
        check_vma=False,
    )
```

```python
import jax
import jax.numpy as jnp
from jax import lax
from jax.experimental import pallas as pl
from jax.experimental.pallas import tpu as pltpu
from jax.sharding import PartitionSpec as P

COL = "col"
ROW_COL = ("row", "col")


slater_cx = 0.7386
kappa_pbe = 0.804
mu_pbe = 0.2195


POINT_BLOCK = 1024
STEPS = 4
LANES = 256
FUNCTIONS = 384


def potentials(density, grad_square):
    inverse_root = jnp.exp(jnp.log(density * density + 1.0) * (-1.0 / 3.0))
    inverse_two = inverse_root * inverse_root
    reduced = grad_square * (inverse_two * inverse_two)
    share = 1.0 / (1.0 + (mu_pbe / kappa_pbe) * reduced)
    enhance = 1.0 + kappa_pbe - kappa_pbe * share
    slope = mu_pbe * share * share
    by_density = (-slater_cx * 4.0 / 3.0) * inverse_root * density * (enhance - 2.0 * reduced * slope)
    by_gradient = -slater_cx * slope * inverse_two
    return by_density, by_gradient


BLOCKS = 64
BAND = 5
HALF = 128
WIDTH = 256
SLICE = 32
PART = 16
COLS = 8
FIRST_PIECES = {
    -2: ((2, 2, 0),),
    -1: ((2, 1, 2), (4, 1, 3)),
    0: ((0, 5, 4),),
    1: ((2, 2, 9),),
    2: ((2, 1, 11),),
}
FIRST_ROLE = {-2: (0, 2), -1: (2, 2), 0: (4, 5), 1: (9, 2), 2: (11, 1)}
FIRST_SLOT = {(-2, -2): 0, (-2, -1): 1, (-1, -1): 2, (-1, 1): 3, (1, 1): 9, (1, 2): 10, (2, 2): 11}
SECOND_ROLE = {-2: (0, 3, 2), -1: (3, 4, 1), 0: (7, 5, 0), 1: (12, 4, 0), 2: (16, 3, 0)}


def first_block(a, b):
    if a == 0:
        return 6 + b, False
    if b == 0:
        return 6 + a, True
    if (a, b) in FIRST_SLOT:
        return FIRST_SLOT[a, b], False
    return FIRST_SLOT[b, a], True


def second_block(a, b):
    return SECOND_ROLE[a][0] + b - max(-2, a - 2), False


def product(left, right, where):
    columns = []
    for b in range(-2, 3):
        total = None
        for a in range(max(-2, b - 2), min(2, b + 2) + 1):
            slot, flipped = where(a, b)
            term = lax.dot_general(
                left(a + 2),
                right[slot],
                (((1,), (1 if flipped else 0,)), ((), ())),
                preferred_element_type=jnp.float32,
            )
            total = term if total is None else total + term
        columns.append(total)
    return columns


def fused_kernel(
    density,
    pattern,
    windows,
    values,
    grads,
    weights,
    purified,
    matrix,
    densities,
    masked,
    kept,
    kept_other,
    starts,
    all_starts,
    start_words,
    natural,
    turned,
    first,
    second,
    squares,
    mine,
    final,
    near,
    ready,
    staged_first,
    staged_second,
    window,
    projected,
    weighted,
    total,
    rows_of,
    terms,
    gathered_first,
    gathered_second,
    sums,
    edges,
    arrived,
    load_sems,
    kept_sems,
    send_starts,
    recv_starts,
    send_first,
    recv_first,
    send_pass,
    recv_pass,
    send_second,
    recv_second,
    send_pass_second,
    recv_pass_second,
    own_sem,
    send_out,
    recv_out,
    send_near,
    recv_near,
    send_window,
    recv_window,
    send_terms,
    recv_terms,
    send_sum,
    recv_sum,
):
    staged, gathered = (staged_first, staged_second), (gathered_first, gathered_second)
    q = lax.axis_index("row")
    c = lax.axis_index("col")
    m = q // 2
    h = q % 2
    j = 2 * (c % 4) + c // 4
    i = 8 * m + j
    rows = pl.ds(pl.multiple_of(HALF * h, HALF), HALF)
    sibling = dict(device_id={"row": 2 * m + 1 - h, "col": c}, device_id_type=pl.DeviceIdType.MESH)

    def chip(block_row):
        return dict(
            device_id={"row": 2 * (block_row // 8) + h, "col": block_row % 2 * 4 + block_row % 8 // 2},
            device_id_type=pl.DeviceIdType.MESH,
        )

    def load(n):
        slot = n % 2
        tile, part = n // STEPS, pl.ds(pl.multiple_of(n % STEPS * POINT_BLOCK, POINT_BLOCK), POINT_BLOCK)
        return (
            pltpu.make_async_copy(values.at[tile, part], natural.at[slot, 0], load_sems.at[slot, 0]),
            pltpu.make_async_copy(grads.at[:, tile, part], natural.at[slot, pl.ds(1, 3)], load_sems.at[slot, 1]),
        )

    for n in range(2):
        for copy in load(n):
            copy.start()

    barrier = pltpu.get_barrier_semaphore()

    def greet(row, col):
        pl.semaphore_signal(
            barrier, inc=1, device_id={"row": row, "col": col}, device_id_type=pl.DeviceIdType.MESH
        )

    @pl.loop(0, COLS)
    def _(other):
        greet(2 * m + 1 - h, other)

        @pl.when(other != c)
        def _():
            greet(q, other)

        @pl.when((m > 0) & (((h == 0) & (other % 4 == 3)) | ((h == 1) & (c % 4 == 0))))
        def _():
            greet(q - 2, other)

        @pl.when((m < 7) & (((h == 1) & (other % 4 == 0)) | ((h == 0) & (c % 4 == 3))))
        def _():
            greet(q + 2, other)

        @pl.when((m > 0) & (h == 0) & ((c == 0) | (other == 7) | (other == c)))
        def _():
            greet(q - 1, other)

        @pl.when((m < 7) & (h == 1) & ((c == 7) | (other == 0) | (other == c)))
        def _():
            greet(q + 1, other)

    lower = jnp.where(m > 0, jnp.where(h == 0, 2, jnp.where(c % 4 == 0, 8, 0)), 0)
    upper = jnp.where(m < 7, jnp.where(h == 1, 2, jnp.where(c % 4 == 3, 8, 0)), 0)
    lower_side = jnp.where((m > 0) & (h == 0), jnp.where(c == 0, 8, jnp.where(c == 7, 1, 2)), 0)
    upper_side = jnp.where((m < 7) & (h == 1), jnp.where(c == 7, 8, jnp.where(c == 0, 1, 2)), 0)

    for local in range(4):
        for d in range(BAND):
            flag = pattern[local, d] > 0
            masked[local, d] = jnp.where(flag, density[local, d], jnp.zeros((SLICE, WIDTH), jnp.bfloat16))
            kept[local, d : d + 1] = jnp.where(flag, jnp.ones((1, WIDTH), jnp.float32), 0.0)
    lane = lax.broadcasted_iota(jnp.int32, (8, 128), 1)
    starts[...] = jnp.where(lane == 0, windows[0], windows[1])
    pl.semaphore_wait(barrier, 15 + lower + upper + lower_side + upper_side)

    def start_copy(other):
        return pltpu.make_async_remote_copy(
            starts,
            all_starts.at[c],
            send_starts.at[other],
            recv_starts,
            device_id={"row": q, "col": other},
            device_id_type=pl.DeviceIdType.MESH,
        )

    @pl.loop(0, COLS)
    def _(other):
        @pl.when(other != c)
        def _():
            start_copy(other).start()

    pltpu.make_async_copy(starts, all_starts.at[c], recv_starts).start()

    kept_copy = pltpu.make_async_remote_copy(
        kept, kept_other, kept_sems.at[0], kept_sems.at[1], **sibling
    )
    kept_copy.start()

    def first_copies(local, act):
        k = 4 * q + local
        place = pl.ds(pl.multiple_of(SLICE * c, SLICE), SLICE)
        index = 0
        for role, pieces in FIRST_PIECES.items():
            target = k - role
            valid = (target >= 0) & (target < BLOCKS)
            for diagonal, count, slot in pieces:
                source = masked.at[local, pl.ds(diagonal, count)]
                landing = first.at[pl.ds(slot, count), place]

                @pl.when(valid & (target != i))
                def _():
                    act(
                        pltpu.make_async_remote_copy(
                            source,
                            landing,
                            send_first.at[local, index],
                            recv_first.at[role + 2],
                            **chip(target),
                        ),
                        True,
                    )

                @pl.when(target == i)
                def _():
                    act(pltpu.make_async_copy(source, landing, recv_first.at[role + 2]), False)

                index += 1

    @pl.loop(0, 4)
    def _(local):
        first_copies(local, lambda copy, remote: copy.start())

    @pl.loop(0, 2 * STEPS)
    def _(n):
        for copy in load(n):
            copy.wait()
        for k in range(4):
            turned[n, k] = natural[n % 2, k].T

        @pl.when(n < 2 * STEPS - 2)
        def _():
            for copy in load(n + 2):
                copy.start()

    def pass_on(role):
        slot, count = FIRST_ROLE[role]
        part = first.at[pl.ds(slot, count)]
        return pltpu.make_async_remote_copy(
            part, part, send_pass.at[role + 2], recv_pass.at[role + 2], **sibling
        )

    order = (0, -1, 1, -2, 2)
    for role in order:
        slot, count = FIRST_ROLE[role]
        part = first.at[pl.ds(slot, count)]
        k = i + role
        valid = (k >= 0) & (k < BLOCKS)

        @pl.when(valid & ((k // 4) % 2 == h))
        def _():
            pltpu.make_async_copy(part, part, recv_first.at[role + 2]).wait()
            pass_on(role).start()

        @pl.when(jnp.logical_not(valid))
        def _():
            first[pl.ds(slot, count)] = jnp.zeros((count, WIDTH, WIDTH), jnp.bfloat16)
            start, number, _ = SECOND_ROLE[role]
            second[pl.ds(start, number)] = jnp.zeros((number, WIDTH, WIDTH), jnp.bfloat16)

    for role in order:
        k = i + role

        @pl.when((k >= 0) & (k < BLOCKS) & ((k // 4) % 2 != h))
        def _():
            pass_on(role).wait_recv()

    kept_copy.wait()
    near_kept = kept[j % 4]
    far_kept = kept_other[j % 4]
    mask = jnp.where(h == j // 4, near_kept, far_kept)

    def iterate(left, right, where, result):
        for d, total in enumerate(product(left, right, where)):
            squares[d] = jnp.where(mask[d : d + 1] > 0, total, 0.0).astype(jnp.bfloat16)
        for d, total in enumerate(product(lambda a: squares[a], right, where)):
            value = 3.0 * squares[d].astype(jnp.float32) - 2.0 * total
            result[d] = jnp.where(mask[d : d + 1] > 0, value, 0.0).astype(jnp.bfloat16)

    iterate(lambda a: first[4 + a, rows, :], first, first_block, mine)

    own = pltpu.make_async_copy(mine, second.at[pl.ds(7, 5), rows], own_sem)
    own.start()
    own_far = pltpu.make_async_remote_copy(
        mine, second.at[pl.ds(7, 5), rows], send_pass_second.at[2], recv_pass_second.at[2], **sibling
    )
    own_far.start()

    def second_copy(role):
        start, number, diagonal = SECOND_ROLE[role]
        return pltpu.make_async_remote_copy(
            mine.at[pl.ds(diagonal, number)],
            second.at[pl.ds(start, number), rows],
            send_second.at[role + 2],
            recv_second.at[role + 2],
            **chip(i - role),
        )

    def second_pass(role):
        start, number, _ = SECOND_ROLE[role]
        part = second.at[pl.ds(start, number), rows]
        return pltpu.make_async_remote_copy(
            part, part, send_pass_second.at[role + 2], recv_pass_second.at[role + 2], **sibling
        )

    others = (-2, 2, -1, 1)
    for role in others:
        target = i - role

        @pl.when((target >= 0) & (target < BLOCKS))
        def _():
            second_copy(role).start()

    for role in (-1, 1, -2, 2):
        k = i + role

        @pl.when((k >= 0) & (k < BLOCKS))
        def _():
            second_copy(role).wait_recv()
            second_pass(role).start()

    for role in (-1, 1, -2, 2):
        k = i + role

        @pl.when((k >= 0) & (k < BLOCKS))
        def _():
            second_pass(role).wait_recv()

    own.wait()
    own_far.wait_recv()
    iterate(lambda a: mine[a], second, second_block, final)

    def out_copies(act):
        for u in range(4):
            source = final.at[:, pl.ds(SLICE * u, SLICE)]
            landing = purified.at[j % 4]
            row, col = 2 * m + j // 4, 4 * h + u
            here = (row == q) & (col == c)

            @pl.when(jnp.logical_not(here))
            def _():
                act(
                    pltpu.make_async_remote_copy(
                        source,
                        landing,
                        send_out.at[u],
                        recv_out.at[j % 4],
                        device_id={"row": row, "col": col},
                        device_id_type=pl.DeviceIdType.MESH,
                    ),
                    True,
                )

            @pl.when(here)
            def _():
                act(pltpu.make_async_copy(source, landing, recv_out.at[j % 4]), False)

    def near_copies(act):
        home = 2 * m + j // 4
        for lane_of, (row, slot, group, needed) in enumerate(
            (
                (home, 2 * (j % 4 + 1) + h, 0, home >= 0),
                (home - 1, 10 + h, 2, (j % 4 == 0) & (home > 0)),
                (home + 1, h, 1, (j % 4 == 3) & (home < 15)),
            )
        ):

            @pl.when(needed)
            def _():
                @pl.loop(0, COLS)
                def _(u):
                    here = (row == q) & (u == c)
                    source = final.at[pl.ds(1, 3), pl.ds(pl.multiple_of(PART * u, PART), PART)]
                    landing = near.at[slot]

                    @pl.when(jnp.logical_not(here))
                    def _():
                        act(
                            pltpu.make_async_remote_copy(
                                source,
                                landing,
                                send_near.at[lane_of, u],
                                recv_near.at[group],
                                device_id={"row": row, "col": u},
                                device_id_type=pl.DeviceIdType.MESH,
                            ),
                            True,
                        )

                    @pl.when(here)
                    def _():
                        act(pltpu.make_async_copy(source, landing, recv_near.at[group]), False)

    near_copies(lambda copy, remote: copy.start())
    pltpu.make_async_copy(all_starts, all_starts, recv_starts).wait()
    words = pltpu.make_async_copy(all_starts, start_words, own_sem)
    words.start()
    words.wait()
    for group, first_slot, count, reached in ((0, 2, 8, q >= 0), (1, 0, 2, q > 0), (2, 10, 2, q < 15)):
        part = near.at[pl.ds(first_slot, count)]

        @pl.when(reached)
        def _():
            pltpu.make_async_copy(part, part, recv_near.at[group]).wait()

        @pl.when(jnp.logical_not(reached))
        def _():
            near[pl.ds(first_slot, count)] = jnp.zeros((count, 3, PART, WIDTH), jnp.bfloat16)

    def window_copy(other, t):
        return pltpu.make_async_remote_copy(
            ready.at[other, t],
            staged[t].at[c],
            send_window.at[other, t],
            recv_window.at[t],
            device_id={"row": q, "col": other},
            device_id_type=pl.DeviceIdType.MESH,
        )

    for t in range(2):

        @pl.loop(1, COLS + 1)
        def _(step):
            other = (c + step) % COLS
            start = start_words[other, 0, t]
            lead = jnp.clip(start - 2 * (4 * q - 1), 0, 9)
            odd = (start % 2) == 1
            for third_row in range(3):
                at = (1, jnp.where(odd, 0, 1), 0)[third_row]
                left = near[lead + third_row, at]
                right = near[lead + third_row, at + 1]
                for third, even_part, odd_part in (
                    (0, left[:, :128], left[:, 128:]),
                    (1, left[:, 128:], right[:, :128]),
                    (2, right[:, :128], right[:, 128:]),
                ):
                    ready[other, t, third_row, :, 128 * third : 128 * third + 128] = jnp.where(
                        odd, odd_part, even_part
                    )

            @pl.when(other != c)
            def _():
                window_copy(other, t).start()

            @pl.when(other == c)
            def _():
                pltpu.make_async_copy(ready.at[other, t], staged[t].at[c], recv_window.at[t]).start()

    out_copies(lambda copy, remote: copy.start())

    def term_copy(other, t):
        return pltpu.make_async_remote_copy(
            terms.at[other, t],
            gathered[t].at[c, pl.ds(0, 2)],
            send_terms.at[other, t],
            recv_terms.at[t],
            device_id={"row": q, "col": other},
            device_id_type=pl.DeviceIdType.MESH,
        )

    for s in range(COLS):
        for t in range(2):
            gathered[t][s, 2] = jnp.zeros((SLICE, FUNCTIONS), jnp.bfloat16)

    rows_of[12] = jnp.zeros((SLICE, FUNCTIONS), jnp.bfloat16)

    for t in range(2):
        part = staged[t]
        pltpu.make_async_copy(part, part, recv_window.at[t]).wait()
        shift = 4 * (start_words[c, 0, t] % 2)
        for third_row in range(3):
            for u in range(COLS):
                place = HALF * third_row + PART * u
                window[place : place + PART, :] = staged[t][u, third_row]
        window[...] = window[...].T
        total[...] = jnp.zeros_like(total)
        weighted[1] = jnp.zeros((FUNCTIONS, POINT_BLOCK), jnp.bfloat16)
        projected[0] = jnp.dot(window[...], turned[STEPS * t, 0], preferred_element_type=jnp.float32)

        @pl.loop(0, STEPS)
        def _(s):
            n = STEPS * t + s
            now, later = s % 2, (s + 1) % 2
            ahead = STEPS * t + jnp.minimum(s + 1, STEPS - 1)
            behind = STEPS * t + jnp.maximum(s - 1, 0)
            projected[later] = jnp.dot(window[...], turned[ahead, 0], preferred_element_type=jnp.float32)
            total[...] += lax.dot_general(
                turned[behind, 0], weighted[later], (((1,), (1,)), ((), ())), preferred_element_type=jnp.float32
            )
            for piece in range(POINT_BLOCK // LANES):
                lanes = slice(piece * LANES, piece * LANES + LANES)
                points = pl.ds(pl.multiple_of(s * POINT_BLOCK + piece * LANES, LANES), LANES)
                x = projected[now, :, lanes]
                reduced = [
                    jnp.sum(x * turned[n, k, :, lanes].astype(jnp.float32), axis=0, keepdims=True)
                    for k in range(4)
                ]
                point_density = reduced[0] / FUNCTIONS
                slopes = [2.0 * r / FUNCTIONS for r in reduced[1:]]
                grad_square = slopes[0] * slopes[0] + slopes[1] * slopes[1] + slopes[2] * slopes[2]
                by_density, by_gradient = potentials(point_density, grad_square)
                densities[t : t + 1, points] = point_density
                scaled = weights[t : t + 1, points] * (1.0 / 4096.0)
                factors = [0.5 * by_density * scaled] + [2.0 * by_gradient * scaled * s for s in slopes]
                z = None
                for k in range(4):
                    factor = jnp.broadcast_to(factors[k], (16, LANES)).astype(jnp.bfloat16)
                    basis = turned[n, k, :, lanes].reshape(FUNCTIONS // 16, 16, LANES)
                    z = factor[None] * basis if z is None else z + factor[None] * basis
                weighted[now, :, lanes] = z.reshape(FUNCTIONS, LANES)

        total[...] += lax.dot_general(
            turned[STEPS * t + STEPS - 1, 0],
            weighted[(STEPS - 1) % 2],
            (((1,), (1,)), ((), ())),
            preferred_element_type=jnp.float32,
        )
        both = total[...] + total[...].T
        for piece in range(12):
            rows_of[piece] = both[SLICE * piece : SLICE * piece + SLICE].astype(jnp.bfloat16)

        @pl.loop(1, COLS + 1)
        def _(step):
            holder = (c + step) % COLS
            for which in range(2):
                piece = holder + 8 * which - shift
                inside = (piece >= 0) & (piece < 12)
                terms[holder, t, which] = rows_of[jnp.where(inside, piece, 12)]

            @pl.when(holder != c)
            def _():
                term_copy(holder, t).start()

            @pl.when(holder == c)
            def _():
                pltpu.make_async_copy(
                    terms.at[holder, t], gathered[t].at[c, pl.ds(0, 2)], recv_terms.at[t]
                ).start()

    def sum_copy(side):
        return pltpu.make_async_remote_copy(
            edges.at[side],
            arrived.at[1 - side],
            send_sum.at[side],
            recv_sum.at[1 - side],
            device_id={"row": q + 2 * side - 1, "col": c},
            device_id_type=pl.DeviceIdType.MESH,
        )

    def add_up(t, lead, which):
        for odd in range(2):
            together = None if t == 0 else sums[lead, which, odd]
            for s in range(COLS):
                start = start_words[s, 0, t]
                chosen = (start // 2 - (4 * q - 1) == lead) & (start % 2 == odd)
                piece = gathered[t][s, jnp.where(chosen, which, 2)].astype(jnp.float32)
                together = piece if together is None else together + piece
            sums[lead, which, odd] = together

    def block_row(r):
        wide = [jnp.zeros((SLICE, HALF), jnp.float32) for _ in range(6)]
        for which in range(2):
            if 0 <= r - which < 5:
                for odd in range(2):
                    piece = sums[r - which, which, odd]
                    for third in range(3):
                        place = 2 + odd - 2 * which + third
                        wide[place] = wide[place] + piece[:, HALF * third : HALF * third + HALF]
        return [jnp.concatenate(wide[2 * d : 2 * d + 2], axis=1) for d in range(3)]

    for t in range(2):
        part = gathered[t].at[:, pl.ds(0, 2)]
        pltpu.make_async_copy(part, part, recv_terms.at[t]).wait()
        add_up(t, 0, 0)
        add_up(t, 4, 1)
        if t == 1:
            for side in range(2):
                for d, block in enumerate(block_row(5 * side)):
                    edges[side, d] = block.astype(jnp.bfloat16)
                reached = (q < 15) if side else (q > 0)

                @pl.when(reached)
                def _():
                    sum_copy(side).start()

        @pl.loop(0, 4)
        def _(lead):
            add_up(t, lead + 1, 0)
            add_up(t, lead, 1)

    for side in range(2):
        reached = (q < 15) if side else (q > 0)

        @pl.when(jnp.logical_not(reached))
        def _():
            arrived[side] = jnp.zeros((3, SLICE, WIDTH), jnp.bfloat16)

    for local in (1, 2, 0, 3):
        if local in (0, 3):
            side = local // 3
            reached = (q < 15) if side else (q > 0)

            @pl.when(reached)
            def _():
                sum_copy(1 - side).wait_recv()

        blocks = block_row(local + 1)
        matrix[local, 0] = jnp.zeros((SLICE, WIDTH), jnp.float32)
        matrix[local, 4] = jnp.zeros((SLICE, WIDTH), jnp.float32)
        for d in range(3):
            block = blocks[d]
            if local in (0, 3):
                block = block + arrived[local // 3, d].astype(jnp.float32)
            matrix[local, d + 1] = jnp.where(pattern[local, d + 1] > 0, block, 0.0)

    for side in range(2):
        reached = (q < 15) if side else (q > 0)

        @pl.when(reached)
        def _():
            sum_copy(side).wait_send()

    @pl.loop(0, 4)
    def _(local):
        first_copies(local, lambda copy, remote: copy.wait_send() if remote else None)

    for role in order:
        k = i + role

        @pl.when((k >= 0) & (k < BLOCKS) & ((k // 4) % 2 == h))
        def _():
            pass_on(role).wait_send()

    own_far.wait_send()
    for role in (-1, 1, -2, 2):
        target = i - role

        @pl.when((target >= 0) & (target < BLOCKS))
        def _():
            second_copy(role).wait_send()

        k = i + role

        @pl.when((k >= 0) & (k < BLOCKS))
        def _():
            second_pass(role).wait_send()

    out_copies(lambda copy, remote: copy.wait_send() if remote else None)
    near_copies(lambda copy, remote: copy.wait_send() if remote else None)
    for local in range(4):
        block = purified.at[local]
        pltpu.make_async_copy(block, block, recv_out.at[local]).wait()

    @pl.loop(0, COLS)
    def _(other):
        @pl.when(other != c)
        def _():
            start_copy(other).wait_send()
            for t in range(2):
                window_copy(other, t).wait_send()
                term_copy(other, t).wait_send()


def hand_over(*refs):
    for source, target in zip(refs[:3], refs[3:]):
        target[...] = source[...]


def on_device(density, pattern, windows, basis_values, basis_grads, weights):
    bf16, f32, dma = jnp.bfloat16, jnp.float32, pltpu.SemaphoreType.DMA
    vmem = pl.BlockSpec(memory_space=pltpu.VMEM)
    smem = pl.BlockSpec(memory_space=pltpu.SMEM)
    hbm = pl.BlockSpec(memory_space=pl.ANY)
    half_row = pltpu.VMEM((BAND, HALF, WIDTH), bf16)
    pieces = pltpu.VMEM((COLS, 2, 2, SLICE, FUNCTIONS), bf16)
    edge = pltpu.VMEM((2, 3, SLICE, WIDTH), bf16)
    results = pl.pallas_call(
        fused_kernel,
        name="fused",
        in_specs=[vmem, smem, smem, hbm, hbm, vmem],
        out_specs=[vmem, vmem, vmem],
        out_shape=[
            jax.ShapeDtypeStruct(density.shape, bf16),
            jax.ShapeDtypeStruct(density.shape, f32),
            jax.ShapeDtypeStruct(weights.shape, f32),
        ],
        scratch_shapes=[
            pltpu.VMEM(density.shape, bf16),
            pltpu.VMEM((4, 8, WIDTH), f32),
            pltpu.VMEM((4, 8, WIDTH), f32),
            pltpu.VMEM((8, 128), jnp.int32),
            pltpu.VMEM((COLS, 8, 128), jnp.int32),
            pltpu.SMEM((COLS, 8, 128), jnp.int32),
            pltpu.VMEM((2, 4, POINT_BLOCK, FUNCTIONS), bf16),
            pltpu.VMEM((2 * STEPS, 4, FUNCTIONS, POINT_BLOCK), bf16),
            pltpu.VMEM((12, WIDTH, WIDTH), bf16),
            pltpu.VMEM((19, WIDTH, WIDTH), bf16),
            half_row,
            half_row,
            half_row,
            pltpu.VMEM((12, 3, PART, WIDTH), bf16),
            pltpu.VMEM((COLS, 2, 3, PART, FUNCTIONS), bf16),
            pltpu.VMEM((COLS, 3, PART, FUNCTIONS), bf16),
            pltpu.VMEM((COLS, 3, PART, FUNCTIONS), bf16),
            pltpu.VMEM((FUNCTIONS, FUNCTIONS), bf16),
            pltpu.VMEM((2, FUNCTIONS, POINT_BLOCK), f32),
            pltpu.VMEM((2, FUNCTIONS, POINT_BLOCK), bf16),
            pltpu.VMEM((FUNCTIONS, FUNCTIONS), f32),
            pltpu.VMEM((13, SLICE, FUNCTIONS), bf16),
            pieces,
            pltpu.VMEM((COLS, 3, SLICE, FUNCTIONS), bf16),
            pltpu.VMEM((COLS, 3, SLICE, FUNCTIONS), bf16),
            pltpu.VMEM((5, 2, 2, SLICE, FUNCTIONS), f32),
            edge,
            edge,
            dma((2, 2)),
            dma((2,)),
            dma((COLS,)),
            dma(()),
            dma((4, 6)),
            dma((5,)),
            dma((5,)),
            dma((5,)),
            dma((5,)),
            dma((5,)),
            dma((5,)),
            dma((5,)),
            dma(()),
            dma((4,)),
            dma((4,)),
            dma((3, COLS)),
            dma((3,)),
            dma((COLS, 2)),
            dma((2,)),
            dma((COLS, 2)),
            dma((2,)),
            dma((2,)),
            dma((2,)),
        ],
        compiler_params=pltpu.CompilerParams(
            collective_id=0, has_side_effects=True, vmem_limit_bytes=63 * 1024 * 1024
        ),
    )(density, pattern, windows, basis_values, basis_grads, weights)
    return pl.pallas_call(
        hand_over,
        name="hand_over",
        in_specs=[vmem, vmem, vmem],
        out_specs=[vmem, vmem, vmem],
        out_shape=[jax.ShapeDtypeStruct(r.shape, r.dtype) for r in results],
    )(*results)


def solution(mesh):
    placed = (
        P("row", None, COL, None),
        P("row", None),
        P(ROW_COL),
        P(ROW_COL, None, None),
        P(None, ROW_COL, None, None),
        P(ROW_COL, None),
    )
    return jax.shard_map(
        on_device,
        mesh=mesh,
        in_specs=placed,
        out_specs=(P("row", None, COL, None), P("row", None, COL, None), P(ROW_COL, None)),
        check_vma=False,
    )
```

```python
import jax
import jax.numpy as jnp
from jax import lax
from jax.experimental import pallas as pl
from jax.experimental.pallas import tpu as pltpu
from jax.sharding import PartitionSpec as P

COL = "col"
ROW_COL = ("row", "col")


slater_cx = 0.7386
kappa_pbe = 0.804
mu_pbe = 0.2195


POINT_BLOCK = 1024
STEPS = 4
LANES = 256
FUNCTIONS = 384


def potentials(density, grad_square):
    inverse_root = jnp.exp(jnp.log(density * density + 1.0) * (-1.0 / 3.0))
    inverse_two = inverse_root * inverse_root
    reduced = grad_square * (inverse_two * inverse_two)
    share = 1.0 / (1.0 + (mu_pbe / kappa_pbe) * reduced)
    enhance = 1.0 + kappa_pbe - kappa_pbe * share
    slope = mu_pbe * share * share
    by_density = (-slater_cx * 4.0 / 3.0) * inverse_root * density * (enhance - 2.0 * reduced * slope)
    by_gradient = -slater_cx * slope * inverse_two
    return by_density, by_gradient


BLOCKS = 64
BAND = 5
HALF = 128
WIDTH = 256
SLICE = 32
PART = 16
COLS = 8
FIRST_PIECES = {
    -2: ((2, 2, 0),),
    -1: ((2, 1, 2), (4, 1, 3)),
    0: ((0, 5, 4),),
    1: ((2, 2, 9),),
    2: ((2, 1, 11),),
}
FIRST_ROLE = {-2: (0, 2), -1: (2, 2), 0: (4, 5), 1: (9, 2), 2: (11, 1)}
FIRST_SLOT = {(-2, -2): 0, (-2, -1): 1, (-1, -1): 2, (-1, 1): 3, (1, 1): 9, (1, 2): 10, (2, 2): 11}
SECOND_ROLE = {-2: (0, 3, 2), -1: (3, 4, 1), 0: (7, 5, 0), 1: (12, 4, 0), 2: (16, 3, 0)}


def first_block(a, b):
    if a == 0:
        return 6 + b, False
    if b == 0:
        return 6 + a, True
    if (a, b) in FIRST_SLOT:
        return FIRST_SLOT[a, b], False
    return FIRST_SLOT[b, a], True


def second_block(a, b):
    return SECOND_ROLE[a][0] + b - max(-2, a - 2), False


def product(left, right, where):
    columns = []
    for b in range(-2, 3):
        total = None
        for a in range(max(-2, b - 2), min(2, b + 2) + 1):
            slot, flipped = where(a, b)
            term = lax.dot_general(
                left(a + 2),
                right[slot],
                (((1,), (1 if flipped else 0,)), ((), ())),
                preferred_element_type=jnp.float32,
            )
            total = term if total is None else total + term
        columns.append(total)
    return columns


def fused_kernel(
    density,
    pattern,
    windows,
    values,
    grads,
    weights,
    purified,
    matrix,
    densities,
    masked,
    kept,
    kept_other,
    starts,
    all_starts,
    start_words,
    natural,
    turned,
    first,
    second,
    squares,
    mine,
    final,
    near,
    ready,
    staged_first,
    staged_second,
    window,
    projected,
    weighted,
    total,
    rows_of,
    terms,
    gathered_first,
    gathered_second,
    sums,
    edges,
    arrived,
    load_sems,
    kept_sems,
    send_starts,
    recv_starts,
    send_first,
    recv_first,
    send_pass,
    recv_pass,
    send_second,
    recv_second,
    send_pass_second,
    recv_pass_second,
    own_sem,
    send_out,
    recv_out,
    send_near,
    recv_near,
    send_window,
    recv_window,
    send_terms,
    recv_terms,
    send_sum,
    recv_sum,
):
    staged, gathered = (staged_first, staged_second), (gathered_first, gathered_second)
    q = lax.axis_index("row")
    c = lax.axis_index("col")
    m = q // 2
    h = q % 2
    j = 2 * (c % 4) + c // 4
    i = 8 * m + j
    rows = pl.ds(pl.multiple_of(HALF * h, HALF), HALF)
    sibling = dict(device_id={"row": 2 * m + 1 - h, "col": c}, device_id_type=pl.DeviceIdType.MESH)

    def chip(block_row):
        return dict(
            device_id={"row": 2 * (block_row // 8) + h, "col": block_row % 2 * 4 + block_row % 8 // 2},
            device_id_type=pl.DeviceIdType.MESH,
        )

    def load(n):
        slot = n % 2
        tile, part = n // STEPS, pl.ds(pl.multiple_of(n % STEPS * POINT_BLOCK, POINT_BLOCK), POINT_BLOCK)
        return (
            pltpu.make_async_copy(values.at[tile, part], natural.at[slot, 0], load_sems.at[slot, 0]),
            pltpu.make_async_copy(grads.at[:, tile, part], natural.at[slot, pl.ds(1, 3)], load_sems.at[slot, 1]),
        )

    for n in range(2):
        for copy in load(n):
            copy.start()

    barrier = pltpu.get_barrier_semaphore()

    def greet(row, col):
        pl.semaphore_signal(
            barrier, inc=1, device_id={"row": row, "col": col}, device_id_type=pl.DeviceIdType.MESH
        )

    @pl.loop(0, COLS)
    def _(other):
        greet(2 * m + 1 - h, other)

        @pl.when(other != c)
        def _():
            greet(q, other)

        @pl.when((m > 0) & (((h == 0) & (other % 4 == 3)) | ((h == 1) & (c % 4 == 0))))
        def _():
            greet(q - 2, other)

        @pl.when((m < 7) & (((h == 1) & (other % 4 == 0)) | ((h == 0) & (c % 4 == 3))))
        def _():
            greet(q + 2, other)

        @pl.when((m > 0) & (h == 0) & ((c == 0) | (other == 7) | (other == c)))
        def _():
            greet(q - 1, other)

        @pl.when((m < 7) & (h == 1) & ((c == 7) | (other == 0) | (other == c)))
        def _():
            greet(q + 1, other)

    lower = jnp.where(m > 0, jnp.where(h == 0, 2, jnp.where(c % 4 == 0, 8, 0)), 0)
    upper = jnp.where(m < 7, jnp.where(h == 1, 2, jnp.where(c % 4 == 3, 8, 0)), 0)
    lower_side = jnp.where((m > 0) & (h == 0), jnp.where(c == 0, 8, jnp.where(c == 7, 1, 2)), 0)
    upper_side = jnp.where((m < 7) & (h == 1), jnp.where(c == 7, 8, jnp.where(c == 0, 1, 2)), 0)

    for local in range(4):
        for d in range(BAND):
            flag = pattern[local, d] > 0
            masked[local, d] = jnp.where(flag, density[local, d], jnp.zeros((SLICE, WIDTH), jnp.bfloat16))
            kept[local, d : d + 1] = jnp.where(flag, jnp.ones((1, WIDTH), jnp.float32), 0.0)
    lane = lax.broadcasted_iota(jnp.int32, (8, 128), 1)
    starts[...] = jnp.where(lane == 0, windows[0], windows[1])
    pl.semaphore_wait(barrier, 15 + lower + upper + lower_side + upper_side)

    def start_copy(other):
        return pltpu.make_async_remote_copy(
            starts,
            all_starts.at[c],
            send_starts.at[other],
            recv_starts,
            device_id={"row": q, "col": other},
            device_id_type=pl.DeviceIdType.MESH,
        )

    @pl.loop(0, COLS)
    def _(other):
        @pl.when(other != c)
        def _():
            start_copy(other).start()

    pltpu.make_async_copy(starts, all_starts.at[c], recv_starts).start()

    kept_copy = pltpu.make_async_remote_copy(
        kept, kept_other, kept_sems.at[0], kept_sems.at[1], **sibling
    )
    kept_copy.start()

    def first_copies(local, act):
        k = 4 * q + local
        place = pl.ds(pl.multiple_of(SLICE * c, SLICE), SLICE)
        index = 0
        for role, pieces in FIRST_PIECES.items():
            target = k - role
            valid = (target >= 0) & (target < BLOCKS)
            for diagonal, count, slot in pieces:
                source = masked.at[local, pl.ds(diagonal, count)]
                landing = first.at[pl.ds(slot, count), place]

                @pl.when(valid & (target != i))
                def _():
                    act(
                        pltpu.make_async_remote_copy(
                            source,
                            landing,
                            send_first.at[local, index],
                            recv_first.at[role + 2],
                            **chip(target),
                        ),
                        True,
                    )

                @pl.when(target == i)
                def _():
                    act(pltpu.make_async_copy(source, landing, recv_first.at[role + 2]), False)

                index += 1

    @pl.loop(0, 4)
    def _(local):
        first_copies(local, lambda copy, remote: copy.start())

    @pl.loop(0, 2 * STEPS)
    def _(n):
        for copy in load(n):
            copy.wait()
        for k in range(4):
            turned[n, k] = natural[n % 2, k].T

        @pl.when(n < 2 * STEPS - 2)
        def _():
            for copy in load(n + 2):
                copy.start()

    def pass_on(role):
        slot, count = FIRST_ROLE[role]
        part = first.at[pl.ds(slot, count)]
        return pltpu.make_async_remote_copy(
            part, part, send_pass.at[role + 2], recv_pass.at[role + 2], **sibling
        )

    order = (0, -1, 1, -2, 2)
    for role in order:
        slot, count = FIRST_ROLE[role]
        part = first.at[pl.ds(slot, count)]
        k = i + role
        valid = (k >= 0) & (k < BLOCKS)

        @pl.when(valid & ((k // 4) % 2 == h))
        def _():
            pltpu.make_async_copy(part, part, recv_first.at[role + 2]).wait()
            pass_on(role).start()

        @pl.when(jnp.logical_not(valid))
        def _():
            first[pl.ds(slot, count)] = jnp.zeros((count, WIDTH, WIDTH), jnp.bfloat16)
            start, number, _ = SECOND_ROLE[role]
            second[pl.ds(start, number)] = jnp.zeros((number, WIDTH, WIDTH), jnp.bfloat16)

    for role in order:
        k = i + role

        @pl.when((k >= 0) & (k < BLOCKS) & ((k // 4) % 2 != h))
        def _():
            pass_on(role).wait_recv()

    kept_copy.wait()
    near_kept = kept[j % 4]
    far_kept = kept_other[j % 4]
    mask = jnp.where(h == j // 4, near_kept, far_kept)

    def iterate(left, right, where, result):
        for d, total in enumerate(product(left, right, where)):
            squares[d] = jnp.where(mask[d : d + 1] > 0, total, 0.0).astype(jnp.bfloat16)
        for d, total in enumerate(product(lambda a: squares[a], right, where)):
            value = 3.0 * squares[d].astype(jnp.float32) - 2.0 * total
            result[d] = jnp.where(mask[d : d + 1] > 0, value, 0.0).astype(jnp.bfloat16)

    iterate(lambda a: first[4 + a, rows, :], first, first_block, mine)

    own = pltpu.make_async_copy(mine, second.at[pl.ds(7, 5), rows], own_sem)
    own.start()
    own_far = pltpu.make_async_remote_copy(
        mine, second.at[pl.ds(7, 5), rows], send_pass_second.at[2], recv_pass_second.at[2], **sibling
    )
    own_far.start()

    def second_copy(role):
        start, number, diagonal = SECOND_ROLE[role]
        return pltpu.make_async_remote_copy(
            mine.at[pl.ds(diagonal, number)],
            second.at[pl.ds(start, number), rows],
            send_second.at[role + 2],
            recv_second.at[role + 2],
            **chip(i - role),
        )

    def second_pass(role):
        start, number, _ = SECOND_ROLE[role]
        part = second.at[pl.ds(start, number), rows]
        return pltpu.make_async_remote_copy(
            part, part, send_pass_second.at[role + 2], recv_pass_second.at[role + 2], **sibling
        )

    others = (-2, 2, -1, 1)
    for role in others:
        target = i - role

        @pl.when((target >= 0) & (target < BLOCKS))
        def _():
            second_copy(role).start()

    for role in (-1, 1, -2, 2):
        k = i + role

        @pl.when((k >= 0) & (k < BLOCKS))
        def _():
            second_copy(role).wait_recv()
            second_pass(role).start()

    for role in (-1, 1, -2, 2):
        k = i + role

        @pl.when((k >= 0) & (k < BLOCKS))
        def _():
            second_pass(role).wait_recv()

    own.wait()
    own_far.wait_recv()
    iterate(lambda a: mine[a], second, second_block, final)

    def out_copies(act):
        for u in range(4):
            source = final.at[:, pl.ds(SLICE * u, SLICE)]
            landing = purified.at[j % 4]
            row, col = 2 * m + j // 4, 4 * h + u
            here = (row == q) & (col == c)

            @pl.when(jnp.logical_not(here))
            def _():
                act(
                    pltpu.make_async_remote_copy(
                        source,
                        landing,
                        send_out.at[u],
                        recv_out.at[j % 4],
                        device_id={"row": row, "col": col},
                        device_id_type=pl.DeviceIdType.MESH,
                    ),
                    True,
                )

            @pl.when(here)
            def _():
                act(pltpu.make_async_copy(source, landing, recv_out.at[j % 4]), False)

    def near_copies(act):
        home = 2 * m + j // 4
        for lane_of, (row, slot, group, needed) in enumerate(
            (
                (home, 2 * (j % 4 + 1) + h, 0, home >= 0),
                (home - 1, 10 + h, 2, (j % 4 == 0) & (home > 0)),
                (home + 1, h, 1, (j % 4 == 3) & (home < 15)),
            )
        ):

            @pl.when(needed)
            def _():
                @pl.loop(0, COLS)
                def _(u):
                    here = (row == q) & (u == c)
                    source = final.at[pl.ds(1, 3), pl.ds(pl.multiple_of(PART * u, PART), PART)]
                    landing = near.at[slot]

                    @pl.when(jnp.logical_not(here))
                    def _():
                        act(
                            pltpu.make_async_remote_copy(
                                source,
                                landing,
                                send_near.at[lane_of, u],
                                recv_near.at[group],
                                device_id={"row": row, "col": u},
                                device_id_type=pl.DeviceIdType.MESH,
                            ),
                            True,
                        )

                    @pl.when(here)
                    def _():
                        act(pltpu.make_async_copy(source, landing, recv_near.at[group]), False)

    near_copies(lambda copy, remote: copy.start())
    pltpu.make_async_copy(all_starts, all_starts, recv_starts).wait()
    words = pltpu.make_async_copy(all_starts, start_words, own_sem)
    words.start()
    words.wait()
    for group, first_slot, count, reached in ((0, 2, 8, q >= 0), (1, 0, 2, q > 0), (2, 10, 2, q < 15)):
        part = near.at[pl.ds(first_slot, count)]

        @pl.when(reached)
        def _():
            pltpu.make_async_copy(part, part, recv_near.at[group]).wait()

        @pl.when(jnp.logical_not(reached))
        def _():
            near[pl.ds(first_slot, count)] = jnp.zeros((count, 3, PART, WIDTH), jnp.bfloat16)

    def window_copy(other, t):
        return pltpu.make_async_remote_copy(
            ready.at[other, t],
            staged[t].at[c],
            send_window.at[other, t],
            recv_window.at[t],
            device_id={"row": q, "col": other},
            device_id_type=pl.DeviceIdType.MESH,
        )

    for t in range(2):

        @pl.loop(1, COLS + 1)
        def _(step):
            other = (c + step) % COLS
            start = start_words[other, 0, t]
            lead = jnp.clip(start - 2 * (4 * q - 1), 0, 9)
            odd = (start % 2) == 1
            for third_row in range(3):
                at = (1, jnp.where(odd, 0, 1), 0)[third_row]
                left = near[lead + third_row, at]
                right = near[lead + third_row, at + 1]
                for third, even_part, odd_part in (
                    (0, left[:, :128], left[:, 128:]),
                    (1, left[:, 128:], right[:, :128]),
                    (2, right[:, :128], right[:, 128:]),
                ):
                    ready[other, t, third_row, :, 128 * third : 128 * third + 128] = jnp.where(
                        odd, odd_part, even_part
                    )

            @pl.when(other != c)
            def _():
                window_copy(other, t).start()

            @pl.when(other == c)
            def _():
                pltpu.make_async_copy(ready.at[other, t], staged[t].at[c], recv_window.at[t]).start()

    out_copies(lambda copy, remote: copy.start())

    def term_copy(other, t):
        return pltpu.make_async_remote_copy(
            terms.at[other, t],
            gathered[t].at[c, pl.ds(0, 2)],
            send_terms.at[other, t],
            recv_terms.at[t],
            device_id={"row": q, "col": other},
            device_id_type=pl.DeviceIdType.MESH,
        )

    for s in range(COLS):
        for t in range(2):
            gathered[t][s, 2] = jnp.zeros((SLICE, FUNCTIONS), jnp.bfloat16)

    rows_of[12] = jnp.zeros((SLICE, FUNCTIONS), jnp.bfloat16)

    for t in range(2):
        part = staged[t]
        pltpu.make_async_copy(part, part, recv_window.at[t]).wait()
        shift = 4 * (start_words[c, 0, t] % 2)
        for third_row in range(3):
            for u in range(COLS):
                place = HALF * third_row + PART * u
                window[place : place + PART, :] = staged[t][u, third_row]
        window[...] = window[...].T
        total[...] = jnp.zeros_like(total)
        weighted[1] = jnp.zeros((FUNCTIONS, POINT_BLOCK), jnp.bfloat16)
        projected[0] = jnp.dot(window[...], turned[STEPS * t, 0], preferred_element_type=jnp.float32)

        @pl.loop(0, STEPS)
        def _(s):
            n = STEPS * t + s
            now, later = s % 2, (s + 1) % 2
            ahead = STEPS * t + jnp.minimum(s + 1, STEPS - 1)
            behind = STEPS * t + jnp.maximum(s - 1, 0)
            projected[later] = jnp.dot(window[...], turned[ahead, 0], preferred_element_type=jnp.float32)
            total[...] += lax.dot_general(
                turned[behind, 0], weighted[later], (((1,), (1,)), ((), ())), preferred_element_type=jnp.float32
            )
            for piece in range(POINT_BLOCK // LANES):
                lanes = slice(piece * LANES, piece * LANES + LANES)
                points = pl.ds(pl.multiple_of(s * POINT_BLOCK + piece * LANES, LANES), LANES)
                x = projected[now, :, lanes]
                reduced = [
                    jnp.sum(x * turned[n, k, :, lanes].astype(jnp.float32), axis=0, keepdims=True)
                    for k in range(4)
                ]
                point_density = reduced[0] / FUNCTIONS
                slopes = [2.0 * r / FUNCTIONS for r in reduced[1:]]
                grad_square = slopes[0] * slopes[0] + slopes[1] * slopes[1] + slopes[2] * slopes[2]
                by_density, by_gradient = potentials(point_density, grad_square)
                densities[t : t + 1, points] = point_density
                scaled = weights[t : t + 1, points] * (1.0 / 4096.0)
                factors = [0.5 * by_density * scaled] + [2.0 * by_gradient * scaled * s for s in slopes]
                z = None
                for k in range(4):
                    factor = jnp.broadcast_to(factors[k], (16, LANES)).astype(jnp.bfloat16)
                    basis = turned[n, k, :, lanes].reshape(FUNCTIONS // 16, 16, LANES)
                    z = factor[None] * basis if z is None else z + factor[None] * basis
                weighted[now, :, lanes] = z.reshape(FUNCTIONS, LANES)

        total[...] += lax.dot_general(
            turned[STEPS * t + STEPS - 1, 0],
            weighted[(STEPS - 1) % 2],
            (((1,), (1,)), ((), ())),
            preferred_element_type=jnp.float32,
        )
        both = total[...] + total[...].T
        for piece in range(12):
            rows_of[piece] = both[SLICE * piece : SLICE * piece + SLICE].astype(jnp.bfloat16)

        @pl.loop(1, COLS + 1)
        def _(step):
            holder = (c + step) % COLS
            for which in range(2):
                piece = holder + 8 * which - shift
                inside = (piece >= 0) & (piece < 12)
                terms[holder, t, which] = rows_of[jnp.where(inside, piece, 12)]

            @pl.when(holder != c)
            def _():
                term_copy(holder, t).start()

            @pl.when(holder == c)
            def _():
                pltpu.make_async_copy(
                    terms.at[holder, t], gathered[t].at[c, pl.ds(0, 2)], recv_terms.at[t]
                ).start()

    def sum_copy(side):
        return pltpu.make_async_remote_copy(
            edges.at[side],
            arrived.at[1 - side],
            send_sum.at[side],
            recv_sum.at[1 - side],
            device_id={"row": q + 2 * side - 1, "col": c},
            device_id_type=pl.DeviceIdType.MESH,
        )

    lowest = 2 * (4 * q - 1)

    def add_up(t, lead, which):
        for odd in range(2):
            together = None if t == 0 else sums[lead, which, odd]
            for s in range(COLS):
                chosen = start_words[s, 0, t] == lowest + 2 * lead + odd
                piece = gathered[t][s, jnp.where(chosen, which, 2)].astype(jnp.float32)
                together = piece if together is None else together + piece
            sums[lead, which, odd] = together

    def block_row(r):
        wide = [jnp.zeros((SLICE, HALF), jnp.float32) for _ in range(6)]
        for which in range(2):
            if 0 <= r - which < 5:
                for odd in range(2):
                    piece = sums[r - which, which, odd]
                    for third in range(3):
                        place = 2 + odd - 2 * which + third
                        wide[place] = wide[place] + piece[:, HALF * third : HALF * third + HALF]
        return [jnp.concatenate(wide[2 * d : 2 * d + 2], axis=1) for d in range(3)]

    for t in range(2):
        part = gathered[t].at[:, pl.ds(0, 2)]
        pltpu.make_async_copy(part, part, recv_terms.at[t]).wait()
        add_up(t, 0, 0)
        add_up(t, 4, 1)
        if t == 1:
            for side in range(2):
                for d, block in enumerate(block_row(5 * side)):
                    edges[side, d] = block.astype(jnp.bfloat16)
                reached = (q < 15) if side else (q > 0)

                @pl.when(reached)
                def _():
                    sum_copy(side).start()

        @pl.loop(0, 4)
        def _(lead):
            add_up(t, lead + 1, 0)
            add_up(t, lead, 1)

    for side in range(2):
        reached = (q < 15) if side else (q > 0)

        @pl.when(jnp.logical_not(reached))
        def _():
            arrived[side] = jnp.zeros((3, SLICE, WIDTH), jnp.bfloat16)

    for local in (1, 2, 0, 3):
        if local in (0, 3):
            side = local // 3
            reached = (q < 15) if side else (q > 0)

            @pl.when(reached)
            def _():
                sum_copy(1 - side).wait_recv()

        blocks = block_row(local + 1)
        matrix[local, 0] = jnp.zeros((SLICE, WIDTH), jnp.float32)
        matrix[local, 4] = jnp.zeros((SLICE, WIDTH), jnp.float32)
        for d in range(3):
            block = blocks[d]
            if local in (0, 3):
                block = block + arrived[local // 3, d].astype(jnp.float32)
            matrix[local, d + 1] = jnp.where(pattern[local, d + 1] > 0, block, 0.0)

    for side in range(2):
        reached = (q < 15) if side else (q > 0)

        @pl.when(reached)
        def _():
            sum_copy(side).wait_send()

    @pl.loop(0, 4)
    def _(local):
        first_copies(local, lambda copy, remote: copy.wait_send() if remote else None)

    for role in order:
        k = i + role

        @pl.when((k >= 0) & (k < BLOCKS) & ((k // 4) % 2 == h))
        def _():
            pass_on(role).wait_send()

    own_far.wait_send()
    for role in (-1, 1, -2, 2):
        target = i - role

        @pl.when((target >= 0) & (target < BLOCKS))
        def _():
            second_copy(role).wait_send()

        k = i + role

        @pl.when((k >= 0) & (k < BLOCKS))
        def _():
            second_pass(role).wait_send()

    out_copies(lambda copy, remote: copy.wait_send() if remote else None)
    near_copies(lambda copy, remote: copy.wait_send() if remote else None)
    for local in range(4):
        block = purified.at[local]
        pltpu.make_async_copy(block, block, recv_out.at[local]).wait()

    @pl.loop(0, COLS)
    def _(other):
        @pl.when(other != c)
        def _():
            start_copy(other).wait_send()
            for t in range(2):
                window_copy(other, t).wait_send()
                term_copy(other, t).wait_send()


def hand_over(*refs):
    for source, target in zip(refs[:3], refs[3:]):
        target[...] = source[...]


def on_device(density, pattern, windows, basis_values, basis_grads, weights):
    bf16, f32, dma = jnp.bfloat16, jnp.float32, pltpu.SemaphoreType.DMA
    vmem = pl.BlockSpec(memory_space=pltpu.VMEM)
    smem = pl.BlockSpec(memory_space=pltpu.SMEM)
    hbm = pl.BlockSpec(memory_space=pl.ANY)
    half_row = pltpu.VMEM((BAND, HALF, WIDTH), bf16)
    pieces = pltpu.VMEM((COLS, 2, 2, SLICE, FUNCTIONS), bf16)
    edge = pltpu.VMEM((2, 3, SLICE, WIDTH), bf16)
    results = pl.pallas_call(
        fused_kernel,
        name="fused",
        in_specs=[vmem, smem, smem, hbm, hbm, vmem],
        out_specs=[vmem, vmem, vmem],
        out_shape=[
            jax.ShapeDtypeStruct(density.shape, bf16),
            jax.ShapeDtypeStruct(density.shape, f32),
            jax.ShapeDtypeStruct(weights.shape, f32),
        ],
        scratch_shapes=[
            pltpu.VMEM(density.shape, bf16),
            pltpu.VMEM((4, 8, WIDTH), f32),
            pltpu.VMEM((4, 8, WIDTH), f32),
            pltpu.VMEM((8, 128), jnp.int32),
            pltpu.VMEM((COLS, 8, 128), jnp.int32),
            pltpu.SMEM((COLS, 8, 128), jnp.int32),
            pltpu.VMEM((2, 4, POINT_BLOCK, FUNCTIONS), bf16),
            pltpu.VMEM((2 * STEPS, 4, FUNCTIONS, POINT_BLOCK), bf16),
            pltpu.VMEM((12, WIDTH, WIDTH), bf16),
            pltpu.VMEM((19, WIDTH, WIDTH), bf16),
            half_row,
            half_row,
            half_row,
            pltpu.VMEM((12, 3, PART, WIDTH), bf16),
            pltpu.VMEM((COLS, 2, 3, PART, FUNCTIONS), bf16),
            pltpu.VMEM((COLS, 3, PART, FUNCTIONS), bf16),
            pltpu.VMEM((COLS, 3, PART, FUNCTIONS), bf16),
            pltpu.VMEM((FUNCTIONS, FUNCTIONS), bf16),
            pltpu.VMEM((2, FUNCTIONS, POINT_BLOCK), f32),
            pltpu.VMEM((2, FUNCTIONS, POINT_BLOCK), bf16),
            pltpu.VMEM((FUNCTIONS, FUNCTIONS), f32),
            pltpu.VMEM((13, SLICE, FUNCTIONS), bf16),
            pieces,
            pltpu.VMEM((COLS, 3, SLICE, FUNCTIONS), bf16),
            pltpu.VMEM((COLS, 3, SLICE, FUNCTIONS), bf16),
            pltpu.VMEM((5, 2, 2, SLICE, FUNCTIONS), f32),
            edge,
            edge,
            dma((2, 2)),
            dma((2,)),
            dma((COLS,)),
            dma(()),
            dma((4, 6)),
            dma((5,)),
            dma((5,)),
            dma((5,)),
            dma((5,)),
            dma((5,)),
            dma((5,)),
            dma((5,)),
            dma(()),
            dma((4,)),
            dma((4,)),
            dma((3, COLS)),
            dma((3,)),
            dma((COLS, 2)),
            dma((2,)),
            dma((COLS, 2)),
            dma((2,)),
            dma((2,)),
            dma((2,)),
        ],
        compiler_params=pltpu.CompilerParams(
            collective_id=0, has_side_effects=True, vmem_limit_bytes=63 * 1024 * 1024
        ),
    )(density, pattern, windows, basis_values, basis_grads, weights)
    return pl.pallas_call(
        hand_over,
        name="hand_over",
        in_specs=[vmem, vmem, vmem],
        out_specs=[vmem, vmem, vmem],
        out_shape=[jax.ShapeDtypeStruct(r.shape, r.dtype) for r in results],
    )(*results)


def solution(mesh):
    placed = (
        P("row", None, COL, None),
        P("row", None),
        P(ROW_COL),
        P(ROW_COL, None, None),
        P(None, ROW_COL, None, None),
        P(ROW_COL, None),
    )
    return jax.shard_map(
        on_device,
        mesh=mesh,
        in_specs=placed,
        out_specs=(P("row", None, COL, None), P("row", None, COL, None), P(ROW_COL, None)),
        check_vma=False,
    )
```
